512 devices in a mesh: grp: 4 (over z_hi, core), lrn: 128 (over x, z_lo, y).
Axes of the slice: x: 4, y: 8, z: 8 (z_hi: 2, z_lo: 4; z = z_hi * 4 + z_lo), core: 2. Of those that a mesh axis runs over, the one named last changes fastest.
Arguments:
- aerosol_mass: float32 [4, 32, 65536], P(None, None, ('grp', 'lrn')), may hold values from 0.001 to 0.1
- size_bins: int32 [4, 32, 65536], P(None, None, ('grp', 'lrn')), may hold values from 0 to 63
- cloud_tau: float32 [32, 65536], P(None, ('grp', 'lrn')), may hold values from 0.02 to 2
- cloud_mask: int32 [65536], P(('grp', 'lrn')), may hold values 0 or 1
- absorber: float32 [32, 65536], P(None, ('grp', 'lrn')), may hold values from 0.3 to 3
- surface_albedo: float32 [14, 65536], P(None, ('grp', 'lrn')), may hold values from 0.05 to 0.85
- cos_zenith: float32 [65536], P(('grp', 'lrn')), may hold values from 0.15 to 1
- ext_table: float32 [112, 256], replicated, may hold values from 0.2 to 2
- ssa_table: float32 [112, 256], replicated, may hold values from 0.5 to 0.95
- asym_table: float32 [112, 256], replicated, may hold values from 0.3 to 0.8
- gas_coeff: float32 [112], replicated, may hold values from 0.001 to 0.5
- solar_flux: float32 [112], replicated, may hold values from 0.3 to 3
- band_map: int32 [112], replicated, may hold values from 0 to 13
- column_learner: int32 [65536, 1], P(('grp', 'lrn')), may hold values from 0 to 127; in each aligned block of 128 rows (0 to 127, 128 to 255, ...) at most 2 rows name the same one
- trunk_weight: bfloat16 [2048, 256], P('lrn'), may hold values from -0.375 to 0.375
- trunk_bias: bfloat16 [2048], P('lrn'), may hold values from -3 to 3
- head_weight: bfloat16 [128, 2048, 128], P('lrn'), may hold values from -0.125 to 0.125
Outputs:
- fluxes: float32 [128, 65536], P(None, ('grp', 'lrn'))
- head_grad: float32 [128, 2048, 128], P('lrn')
- trunk_grad: float32 [2048, 256], P('lrn')
- bias_grad: float32 [2048], P('lrn')
The draws below stay inside these ranges and needn't reach their ends.
Inputs may be any that keep to these rules, and one draw needn't show every extreme that they name: `column_learner`: in each aligned block of 128 rows (the columns of one device) no learner is named more than 2 times, a bound that some block reaches.
All inputs are finite; a program needn't handle non-finite values. No bound on the sum of `cloud_mask` on one device may be relied on, other than what follows from the above.
Results may differ from the reference program's by a relative error of at most 0.0019.
Values may be sent and summed in bfloat16 or wider, within the bound.
A program may use at most 64 MiB of HBM per device.

```python
import math
from functools import partial
import jax
import jax.numpy as jnp
import numpy as np
from jax import lax

MODES = 4
BINS = 64
G = 112
NB = 14
LEV = 32
H = 2048
COL_DEV = 128
COLUMNS = 65536
CAP = 2
IN = 256
OUT = 128
N_GRP = 4
N_LRN = 128


def with_ends(values, rng, low, largest):
    longest = values.shape.index(max(values.shape))
    spots = []
    for shift in (0, 1):
        where = [jax.random.randint(jax.random.fold_in(rng, axis), (), 0, length) for axis, length in enumerate(values.shape)]
        where[longest] = (where[longest] + shift) % values.shape[longest]
        spots.append(tuple(where))
    return values.at[spots[0]].set(low).at[spots[1]].set(largest)


def level_of(own_key, shape, cuts, low, top_value):
    def one(axis_at, parts):
        steps = jax.random.uniform(jax.random.fold_in(jax.random.fold_in(own_key, 6), axis_at), (parts,), jnp.float32, low / len(cuts), top_value / len(cuts))
        return jnp.repeat(jnp.exp(steps), shape[axis_at] // parts).reshape((-1,) + (1,) * (len(shape) - axis_at - 1))

    gain = one(*cuts[0])
    for cut in cuts[1:]:
        gain = gain * one(*cut)
    return gain


def deal_out(key, own, number, rows, number_of, top, most, skew):
    order = jax.random.permutation(key, number_of)
    packed, ordinary = load_shares(number_of, rows * top, most, skew, True), load_shares(number_of, rows * top, most, skew, False)
    places = jnp.arange(number_of)

    def named(lengths, offset_by):
        used = int((lengths > 0).sum())
        fixed = max(1, used // 4)
        shifted = fixed + (places - fixed + offset_by * (used - fixed)) % max(1, number_of - fixed)
        return jnp.zeros((number_of,), jnp.int32).at[order[jnp.where(places < fixed, places, shifted)]].set(jnp.asarray(lengths, jnp.int32))

    lengths = jnp.where(number % 4 == 0, named(packed, number // 4), named(ordinary, number - number // 4 - 1))
    mixed = jax.random.permutation(jax.random.fold_in(own, 3), number_of)
    giver, receiver = mixed[0:number_of // 2 * 2:2], mixed[1:number_of // 2 * 2:2]
    slack = jnp.minimum(lengths[giver] - 1, most - lengths[receiver]) // 2
    slack = jnp.where((giver == order[0]) | (receiver == order[0]) | (lengths[receiver] == 0), 0, jnp.maximum(slack, 0))
    shifted = jax.random.randint(jax.random.fold_in(own, 4), (number_of // 2,), 0, 1 << 20) % (slack + 1)
    lengths = lengths.at[giver].add(-shifted).at[receiver].add(shifted)
    members = jnp.searchsorted(jnp.cumsum(lengths), jnp.arange(rows * top), side="right").astype(jnp.int32)
    listing = members.reshape(top, rows).T
    listing = listing[jax.random.permutation(jax.random.fold_in(own, 1), rows)]
    offset_by = jax.random.randint(jax.random.fold_in(own, 2), (rows, 1), 0, top)
    return jnp.take_along_axis(listing, (jnp.arange(top)[None, :] + offset_by) % top, axis=1)


def load_shares(amount, total, limit, skew, full):
    portions = [(1 << 20) // math.isqrt(rank ** skew) + 1 for rank in range(1, amount + 1)]
    largest = limit if full else min(limit, max(-(-total // amount), total * portions[0] // sum(portions)))
    least = 1 if total - largest >= amount - 1 else 0
    holding, surplus = [largest] + [least] * (amount - 1), total - largest - least * (amount - 1)
    while surplus > 0:
        movable = [i for i in range(1, amount) if holding[i] < largest] or [i for i in range(1, amount) if holding[i] < limit]
        mass, budget = sum([portions[i] for i in movable]), surplus
        for i in movable:
            more = min(limit - holding[i], max(1, budget * portions[i] // mass), surplus)
            holding[i] = holding[i] + more
            surplus = surplus - more
    return np.array(holding)


def bell_draw(stream_key, shape, deviation, limit, shards=(), kind=jnp.bfloat16):
    drawn = deviation * jax.random.normal(stream_key, shape, jnp.float32)
    if shards:
        drawn = drawn * level_of(stream_key, shape, shards, -0.22, 0.18)
    return jnp.clip(drawn, -limit, limit).astype(kind)


def setup_inputs(seed: int = 0) -> dict:
    keys = jax.random.split(jax.random.key(seed), 18)
    aerosol_mass = jnp.clip(jnp.exp(math.log(0.1) - 4.6051702 * jax.random.uniform(keys[0], (MODES, LEV, COLUMNS), jnp.float32) ** level_of(keys[0], (MODES, LEV, COLUMNS), ((2, 512),), -0.2, 0.2)), 0.001, 0.1)
    size_bins = with_ends(jax.random.randint(keys[1], (MODES, LEV, COLUMNS), 0, BINS), jax.random.fold_in(keys[1], 1), 0, BINS - 1).astype(jnp.int32)
    cloud_tau = jnp.clip(jnp.exp(math.log(2.0) - 4.6051702 * jax.random.uniform(keys[2], (LEV, COLUMNS), jnp.float32) ** level_of(keys[2], (LEV, COLUMNS), ((1, 512),), -0.2, 0.2)), 0.02, 2.0)
    cloud_mask = with_ends((jax.random.randint(keys[3], (COLUMNS,), 0, 3) < 1).astype(jnp.int32), jax.random.fold_in(keys[3], 1), 0, 1)
    absorber = jnp.clip(jnp.exp(math.log(3.0) - 2.3025851 * jax.random.uniform(keys[4], (LEV, COLUMNS), jnp.float32) ** level_of(keys[4], (LEV, COLUMNS), ((1, 512),), -0.2, 0.2)), 0.3, 3.0)
    surface_albedo = jnp.clip(0.05 + 0.8 * jax.random.uniform(keys[5], (NB, COLUMNS), jnp.float32) ** level_of(keys[5], (NB, COLUMNS), ((1, 512),), -0.2, 0.2), 0.05, 0.85)
    cos_zenith = jnp.clip(0.15 + 0.85 * jax.random.uniform(keys[6], (COLUMNS,), jnp.float32) ** level_of(keys[6], (COLUMNS,), ((0, 512),), -0.2, 0.2), 0.15, 1.0)
    ext_table = jnp.clip(jnp.exp(jax.random.uniform(keys[7], (G, MODES * BINS), jnp.float32, math.log(0.2), math.log(2.0))), 0.2, 2.0)
    ssa_table = jnp.clip(jax.random.uniform(keys[8], (G, MODES * BINS), jnp.float32, 0.5, 0.95), 0.5, 0.95)
    asym_table = jnp.clip(jax.random.uniform(keys[9], (G, MODES * BINS), jnp.float32, 0.3, 0.8), 0.3, 0.8)
    gas_coeff = jnp.clip(jnp.exp(jax.random.uniform(keys[10], (G,), jnp.float32, math.log(0.001), math.log(0.5))), 0.001, 0.5)
    solar_flux = jnp.clip(jnp.exp(jax.random.uniform(keys[11], (G,), jnp.float32, math.log(0.3), math.log(3.0))), 0.3, 3.0)
    band_map = with_ends(jax.random.randint(keys[12], (G,), 0, NB), jax.random.fold_in(keys[12], 1), 0, NB - 1).astype(jnp.int32)
    column_learner_keys = jax.random.split(jax.random.fold_in(keys[13], 1), COLUMNS // COL_DEV)
    column_learner_turns = jax.random.permutation(jax.random.fold_in(keys[13], 3), COLUMNS // COL_DEV)
    column_learner = jax.vmap(lambda own, number: deal_out(jax.random.fold_in(keys[13], 2), own, number, COL_DEV, N_LRN, 1, CAP, 2))(column_learner_keys, column_learner_turns).reshape((COLUMNS, 1))
    trunk_weight = bell_draw(keys[14], (H, IN), IN ** -0.5, 0.375, ((0, 128),))
    trunk_bias = bell_draw(keys[15], (H,), 0.5, 3.0, ((0, 128),))
    head_weight = bell_draw(keys[16], (N_LRN, H, OUT), H ** -0.5, 0.125, ((0, 128),))
    return {"aerosol_mass": aerosol_mass, "size_bins": size_bins, "cloud_tau": cloud_tau, "cloud_mask": cloud_mask, "absorber": absorber, "surface_albedo": surface_albedo, "cos_zenith": cos_zenith, "ext_table": ext_table, "ssa_table": ssa_table, "asym_table": asym_table, "gas_coeff": gas_coeff, "solar_flux": solar_flux, "band_map": band_map, "column_learner": column_learner, "trunk_weight": trunk_weight, "trunk_bias": trunk_bias, "head_weight": head_weight}


CLOUD_SSA = 0.99
CLOUD_ASYM = 0.85
PRECISE = lax.Precision.HIGHEST

def optics_table(ext_table, ssa_table, asym_table):
    scatter = ext_table * ssa_table
    return jnp.concatenate([ext_table, scatter, scatter * asym_table], axis=0).astype(jnp.bfloat16)

def column_block(optic_table, gas_coeff, solar_flux, band_map, aerosol_mass, size_bins, cloud_tau, cloud_mask, absorber, surface_albedo, cos_zenith):
    mode_count, levels, width_cols = aerosol_mass.shape
    point_count = gas_coeff.shape[0]
    bin_count = optic_table.shape[1] // mode_count
    band_count = surface_albedo.shape[0]
    labels = jnp.arange(bin_count, dtype=jnp.int32)
    load_bf = aerosol_mass.astype(jnp.bfloat16)
    weights = jnp.where(size_bins[:, None] == labels[None, :, None, None], load_bf[:, None], jnp.zeros((), jnp.bfloat16))
    weights = weights.reshape(mode_count * bin_count, levels * width_cols)
    optics = jnp.dot(optic_table, weights, preferred_element_type=jnp.float32).reshape(3, point_count, levels, width_cols)
    cloudy = (cloud_tau * cloud_mask.astype(jnp.float32)[None, :])[None]
    optical_depth = optics[0] + cloudy + gas_coeff[:, None, None] * absorber[None]
    scatter = optics[1] + CLOUD_SSA * cloudy
    forward = optics[2] + CLOUD_SSA * CLOUD_ASYM * cloudy
    single_albedo = scatter / optical_depth
    asym_factor = forward / scatter
    gamma_one = 2.0 - single_albedo * (1.0 + asym_factor)
    gamma_two = single_albedo * (1.0 - asym_factor)
    decay_rate = jnp.sqrt((gamma_one - gamma_two) * (gamma_one + gamma_two))
    damped = jnp.exp(-decay_rate * optical_depth)
    square = damped * damped
    denominator = decay_rate + gamma_one + (decay_rate - gamma_one) * square
    reflect = jnp.moveaxis(gamma_two * (1.0 - square) / denominator, 1, 0)
    transmit = jnp.moveaxis(2.0 * decay_rate * damped / denominator, 1, 0)
    band_hot = (band_map[:, None] == jnp.arange(band_count, dtype=jnp.int32)[None, :]).astype(jnp.float32)
    surface = jnp.dot(band_hot, surface_albedo, precision=PRECISE)
    source = solar_flux[:, None] * cos_zenith[None, :]

    def upward(below_reflect, layer):
        layer_reflect, layer_transmit = layer
        above = layer_reflect + layer_transmit * layer_transmit * below_reflect / (1.0 - layer_reflect * below_reflect)
        return (above, below_reflect)
    top_reflect, below_all = lax.scan(upward, surface, (reflect, transmit), reverse=True)

    def downward(down_now, layer):
        layer_reflect, layer_transmit, below_reflect = layer
        down_next = layer_transmit * down_now / (1.0 - layer_reflect * below_reflect)
        return (down_next, (down_next, below_reflect * down_next))
    _, (down_all, up_all) = lax.scan(downward, source, (reflect, transmit, below_all))
    upper = jnp.concatenate([(top_reflect * source)[None], up_all[:-1]], axis=0)
    group_hot = jnp.stack([band_map < band_count // 2, band_map >= band_count // 2]).astype(jnp.float32) * (2.0 / point_count)
    down_flux = jnp.einsum('kg,lgc->klc', group_hot, down_all, precision=PRECISE)
    up_flux = jnp.einsum('kg,lgc->klc', group_hot, upper, precision=PRECISE)
    return jnp.stack([down_flux, up_flux], axis=1).reshape(4 * levels, width_cols)

def evolve(optic_table, gas_coeff, solar_flux, band_map, aerosol_mass, size_bins, cloud_tau, cloud_mask, absorber, surface_albedo, cos_zenith):
    total_cols = aerosol_mass.shape[-1]
    block_size = min(total_cols, 256)
    block_count = total_cols // block_size

    def splitter(array_in):
        return jnp.moveaxis(array_in.reshape(array_in.shape[:-1] + (block_count, block_size)), -2, 0)
    pieces = tuple((splitter(array_in) for array_in in (aerosol_mass, size_bins, cloud_tau, cloud_mask, absorber, surface_albedo, cos_zenith)))

    def column_job(piece):
        return column_block(optic_table, gas_coeff, solar_flux, band_map, piece[0], piece[1], piece[2], piece[3], piece[4], piece[5], piece[6])
    results = lax.map(column_job, pieces)
    return jnp.moveaxis(results, 0, 1).reshape(results.shape[1], total_cols)

def column_features(aerosol_mass, size_bins, bin_count):
    mode_count, levels, total_cols = aerosol_mass.shape
    first = (jnp.log(aerosol_mass) + 4.6) / 1.4
    second = (size_bins.astype(jnp.float32) - bin_count / 2) / (bin_count / 2)
    stacked = jnp.concatenate([first.reshape(mode_count * levels, total_cols), second.reshape(mode_count * levels, total_cols)], axis=0)
    return stacked.astype(jnp.bfloat16)

def learner_terms(slot_rows, slot_goals, slot_valid, w_full, b_full, w_head, loss_scale):
    pre_act = jnp.dot(slot_rows, w_full.T, preferred_element_type=jnp.float32) + b_full.astype(jnp.float32)[None, :]
    active, slope = jax.vjp(partial(jax.nn.gelu, approximate=True), pre_act)
    hidden = active.astype(jnp.bfloat16)
    predicted = jnp.dot(hidden, w_head, preferred_element_type=jnp.float32)
    error_rows = (predicted - slot_goals.astype(jnp.float32)) * slot_valid.astype(jnp.float32)[:, None]
    pred_grad = (error_rows * loss_scale).astype(jnp.bfloat16)
    hidden_grad = jnp.dot(pred_grad, w_head.T, preferred_element_type=jnp.float32)
    pre_grad = slope(hidden_grad)[0].astype(jnp.bfloat16)
    trunk_part = jnp.dot(pre_grad.T, slot_rows, preferred_element_type=jnp.float32)
    bias_part = lax.optimization_barrier(jnp.sum(pre_grad, axis=0, dtype=jnp.float32))
    return (hidden, pred_grad, trunk_part, bias_part)

def reference(aerosol_mass, size_bins, cloud_tau, cloud_mask, absorber, surface_albedo, cos_zenith, ext_table, ssa_table, asym_table, gas_coeff, solar_flux, band_map, column_learner, trunk_weight, trunk_bias, head_weight):
    optic_table = optics_table(ext_table, ssa_table, asym_table)
    fluxes = evolve(optic_table, gas_coeff, solar_flux, band_map, aerosol_mass, size_bins, cloud_tau, cloud_mask, absorber, surface_albedo, cos_zenith)
    features = column_features(aerosol_mass, size_bins, BINS)
    targets = fluxes.astype(jnp.bfloat16)
    slot_count = N_LRN * CAP
    destination = column_learner[:, 0].reshape(N_GRP * N_LRN, COL_DEV)
    dest_hot = (destination[:, :, None] == jnp.arange(N_LRN, dtype=jnp.int32)[None, None, :]).astype(jnp.int32)
    slot_rank = lax.optimization_barrier(jnp.sum((jnp.cumsum(dest_hot, axis=1) - dest_hot) * dest_hot, axis=2))
    sender = jnp.arange(N_GRP * N_LRN, dtype=jnp.int32)[:, None]
    group_of = sender // N_LRN
    source_of = sender % N_LRN
    slot_index = ((group_of * N_LRN + destination) * slot_count + source_of * CAP + slot_rank).reshape(-1).astype(jnp.int32)
    all_slots = N_GRP * N_LRN * slot_count
    slot_rows = jnp.zeros((all_slots, IN), jnp.bfloat16).at[slot_index].set(features.T)
    slot_goals = jnp.zeros((all_slots, OUT), jnp.bfloat16).at[slot_index].set(targets.T)
    slot_valid = jnp.zeros((all_slots,), jnp.bfloat16).at[slot_index].set(jnp.ones((COLUMNS,), jnp.bfloat16))
    slot_rows = jnp.transpose(slot_rows.reshape(N_GRP, N_LRN, slot_count, IN), (1, 0, 2, 3)).reshape(N_LRN, N_GRP * slot_count, IN)
    slot_goals = jnp.transpose(slot_goals.reshape(N_GRP, N_LRN, slot_count, OUT), (1, 0, 2, 3)).reshape(N_LRN, N_GRP * slot_count, OUT)
    slot_valid = jnp.transpose(slot_valid.reshape(N_GRP, N_LRN, slot_count), (1, 0, 2)).reshape(N_LRN, N_GRP * slot_count)

    def learn_step(totals, inputs_now):
        rows_now, goals_now, valid_now, head_now = inputs_now
        hidden, pred_grad, trunk_part, bias_part = learner_terms(rows_now, goals_now, valid_now, trunk_weight, trunk_bias, head_now, 1.0 / COL_DEV)
        head_part = jnp.dot(hidden.T, pred_grad, preferred_element_type=jnp.float32)
        return ((totals[0] + trunk_part, totals[1] + bias_part), head_part)
    start_sum = (jnp.zeros((H, IN), jnp.float32), jnp.zeros((H,), jnp.float32))
    (trunk_grad, bias_grad), head_grad = lax.scan(learn_step, start_sum, (slot_rows, slot_goals, slot_valid, head_weight))
    return (fluxes, head_grad, trunk_grad, bias_grad)
```

```python
from functools import partial
import math

import jax
import jax.numpy as jnp
from jax import lax
from jax.sharding import Mesh
from jax.experimental import pallas as pl
from jax.experimental.pallas import tpu as pltpu
from jax.sharding import PartitionSpec as P

MODES = 4
BINS = 64
G = 112
NB = 14
LEV = 32
COL_DEV = 128
LRN = ("lrn_0", "lrn_1", "lrn_2")
GRP_LRN = ("grp", "lrn_0", "lrn_1", "lrn_2")


CLOUD_SSA = 0.99
CLOUD_ASYM = 0.85


def in_one_piece(arrays, axis, split_dim, concat_dim, along):
    columns = [a.reshape(*a.shape[:along], -1) for a in arrays]
    both = jnp.concatenate(columns, axis=along)
    whole, at, gathered = (
        lax.all_to_all(both, axis, split_axis=split_dim, concat_axis=concat_dim, tiled=True),
        0,
        [],
    )
    for a, column in zip(arrays, columns):
        piece = whole[..., at : at + column.shape[along]]
        gathered.append(piece.reshape(*piece.shape[:along], *a.shape[along:]))
        at += column.shape[along]
    return tuple(gathered)


def from_everyone(x, axis):
    devices = lax.axis_size(axis)
    return lax.all_to_all(jnp.broadcast_to(x[None], (devices, *x.shape)), axis, 0, 0, tiled=True)


def joined_along(pieces, dim):
    lengths = list(pieces.shape[1:])
    lengths[dim] *= pieces.shape[0]
    return jnp.moveaxis(pieces, 0, dim).reshape(lengths)


def gathered_by_axis(x, axes, dim):
    far, near = axes
    pieces = from_everyone(from_everyone(x, far), near)
    return joined_along(pieces.swapaxes(0, 1).reshape(-1, *x.shape), dim)


def in_one_piece_2(arrays, axis, dim, along):
    columns = [a.reshape(*a.shape[:along], -1) for a in arrays]
    both = jnp.concatenate(columns, axis=along)
    whole, at, gathered = (gathered_by_axis(both, axis, dim), 0, [])
    for a, column in zip(arrays, columns):
        piece = whole[..., at : at + column.shape[along]]
        gathered.append(piece.reshape(*piece.shape[:along], *a.shape[along:]))
        at += column.shape[along]
    return tuple(gathered)


def in_blocks(x, dim, devices):
    lengths = x.shape
    pieces = x.reshape(*lengths[:dim], devices, lengths[dim] // devices, *lengths[dim + 1 :])
    return jnp.moveaxis(pieces, dim, 0)


def sent_and_summed(x, axis, dim):
    devices = lax.axis_size(axis)
    pieces = lax.all_to_all(in_blocks(x, dim, devices), axis, 0, 0, tiled=True)
    return jnp.sum(pieces, axis=0)


def collect(x, axis, dim):
    return joined_along(from_everyone(x, axis), dim)


def sent_and_summed_2(x, axis, dim):
    pieces = in_blocks(x, dim, lax.axis_size(axis))
    arrived = lax.all_to_all(pieces, axis, split_axis=0, concat_axis=0, tiled=True)
    return arrived.astype(jnp.float32).sum(axis=0)


def summed_rows(x, axes, dim):
    far, near = axes
    pieces = in_blocks(x, dim, lax.axis_size(far))
    nearer = sent_and_summed_2(pieces, near, dim + 1)
    arrived = lax.all_to_all(
        nearer.astype(jnp.bfloat16), far, split_axis=0, concat_axis=0, tiled=True
    )
    return arrived.astype(jnp.float32).sum(axis=0)


def in_one_piece_3(arrays, axis, dim, along):
    widths = [math.prod(a.shape[along:]) for a in arrays]
    both = jnp.concatenate(
        [a.reshape(*a.shape[:along], w) for a, w in zip(arrays, widths)], axis=along
    )
    whole = summed_rows(both, axis, dim)
    pieces = jnp.split(whole, [sum(widths[:k]) for k in range(1, len(widths))], axis=along)
    return tuple(
        (b.reshape(*whole.shape[:along], *a.shape[along:]) for a, b in zip(arrays, pieces))
    )


def taken_together(x, axis):
    return from_everyone(x, axis).sum(axis=0)


def packed_total(arrays, axis):
    ravelled, at, gathered = (jnp.concatenate([a.reshape(-1) for a in arrays]), 0, [])
    total = taken_together(ravelled, axis)
    for a in arrays:
        gathered.append(total[at : at + a.size].reshape(a.shape))
        at += a.size
    return tuple(gathered)


def row_to_col(row):
    n = row.shape[1]
    rows = lax.broadcasted_iota(jnp.int32, (n, n), 0)
    cols = lax.broadcasted_iota(jnp.int32, (n, n), 1)
    return jnp.sum(jnp.where(rows == cols, jnp.broadcast_to(row, (n, n)), 0.0), axis=1, keepdims=True)


def evolve_setup(ext, ssa, asy, gas, sol, band, tab, gcol, m0):
    e = ext[...]
    s = e * ssa[...]
    tab[0:G, :] = e.astype(jnp.bfloat16)
    tab[G : 2 * G, :] = s.astype(jnp.bfloat16)
    tab[2 * G : 3 * G, :] = (s * asy[...]).astype(jnp.bfloat16)
    gcol[...] = jnp.broadcast_to(row_to_col(gas[...]), (G, COL_DEV))
    bcol = row_to_col(band[...].astype(jnp.float32))
    m0[...] = jnp.broadcast_to(jnp.where(bcol < NB // 2, 1.0, 0.0), (G, COL_DEV))
    return bcol


CH = 8
LU = 4


def evolve_layers(mass, bins, tau, mask, absb, tab, gcol, opt, refl, trans):
    labels = lax.broadcasted_iota(jnp.int32, (BINS, COL_DEV), 0)
    cloudy_on = mask[...].astype(jnp.float32)

    def body(step, carry):
        pieces = []
        for u in range(LU):
            l = step * LU + u
            modes = []
            for m in range(MODES):
                load = mass[m, pl.ds(l, 1), :]
                hot = bins[m, pl.ds(l, 1), :] == labels
                modes.append(jnp.where(hot, jnp.broadcast_to(load, (BINS, COL_DEV)), 0.0))
            pieces.append(jnp.concatenate(modes, axis=0).astype(jnp.bfloat16))
        weights = jnp.concatenate(pieces, axis=1)
        opt[...] = jnp.dot(tab[...], weights, preferred_element_type=jnp.float32)
        for u in range(LU):
            l = step * LU + u
            cl = tau[pl.ds(l, 1), :] * cloudy_on
            ab = absb[pl.ds(l, 1), :]
            c1 = CLOUD_SSA * cl
            c2 = CLOUD_SSA * CLOUD_ASYM * cl
            lanes = slice(u * COL_DEV, (u + 1) * COL_DEV)
            for g in range(0, G, CH):
                d = opt[g : g + CH, lanes] + cl + gcol[g : g + CH, :] * ab
                s = opt[G + g : G + g + CH, lanes] + c1
                f = opt[2 * G + g : 2 * G + g + CH, lanes] + c2
                ds, df = d - s, d - f
                k = 2.0 * jnp.sqrt(ds * df)
                g1 = ds + df
                e = jnp.exp(-k)
                sq = e * e
                r = 1.0 / ((k + g1) + (k - g1) * sq)
                refl[l, g : g + CH, :] = (s - f) * (1.0 - sq) * r
                trans[l, g : g + CH, :] = 2.0 * k * e * r
        return carry

    lax.fori_loop(0, LEV // LU, body, 0)


def evolve_up(alb, bcol, refl, trans, below):
    surface = jnp.zeros((G, COL_DEV), jnp.float32)
    for b in range(NB):
        surface = jnp.where(bcol == float(b), jnp.broadcast_to(alb[b : b + 1, :], (G, COL_DEV)), surface)
    below[LEV] = surface

    def body(step, carry):
        l = LEV - 1 - step
        for g in range(0, G, CH):
            rows = slice(g, g + CH)
            b = below[l + 1, rows, :]
            r = refl[l, rows, :]
            t = trans[l, rows, :]
            q = t / (1.0 - r * b)
            below[l, rows, :] = r + t * b * q
            trans[l, rows, :] = q
        return carry

    lax.fori_loop(0, LEV, body, 0)


def evolve_down(sol, cosz, m0, below, trans, down, flux):
    cosv = cosz[...]
    scol = row_to_col(sol[...])
    down[...] = jnp.broadcast_to(scol, (G, COL_DEV)) * cosv
    scale = 2.0 / G

    def body(l, carry):
        acc = [jnp.zeros((CH, COL_DEV), jnp.float32) for _ in range(4)]
        for g in range(0, G, CH):
            rows = slice(g, g + CH)
            now = down[rows, :]
            low = m0[rows, :]
            up = below[l, rows, :] * now
            nxt = trans[l, rows, :] * now
            down[rows, :] = nxt
            nl, ul = nxt * low, up * low
            acc[0] = acc[0] + nl
            acc[1] = acc[1] + ul
            acc[2] = acc[2] + (nxt - nl)
            acc[3] = acc[3] + (up - ul)
        for i in range(4):
            flux[pl.ds(i * LEV + l, 1), :] = jnp.sum(acc[i], axis=0, keepdims=True) * scale
        return carry

    lax.fori_loop(0, LEV, body, 0)


def evolve_kernel(mass, bins, tau, mask, absb, alb, cosz, ext, ssa, asy, gas, sol, band, flux,
                  tab, gcol, m0, opt, refl, trans, below, down):
    bcol = evolve_setup(ext, ssa, asy, gas, sol, band, tab, gcol, m0)
    evolve_layers(mass, bins, tau, mask, absb, tab, gcol, opt, refl, trans)
    evolve_up(alb, bcol, refl, trans, below)
    evolve_down(sol, cosz, m0, below, trans, down, flux)


def evolve(mass, bins, tau, mask, absb, alb, cosz, ext, ssa, asy, gas, sol, band):
    return pl.pallas_call(
        evolve_kernel,
        out_shape=jax.ShapeDtypeStruct((4 * LEV, COL_DEV), jnp.float32),
        scratch_shapes=[
            pltpu.VMEM((3 * G, MODES * BINS), jnp.bfloat16),
            pltpu.VMEM((G, COL_DEV), jnp.float32),
            pltpu.VMEM((G, COL_DEV), jnp.float32),
            pltpu.VMEM((3 * G, LU * COL_DEV), jnp.float32),
            pltpu.VMEM((LEV, G, COL_DEV), jnp.float32),
            pltpu.VMEM((LEV, G, COL_DEV), jnp.float32),
            pltpu.VMEM((LEV + 1, G, COL_DEV), jnp.float32),
            pltpu.VMEM((G, COL_DEV), jnp.float32),
        ],
        cost_estimate=pl.CostEstimate(flops=10**9, bytes_accessed=10**6, transcendentals=10**6),
    )(mass, bins, tau, mask[None], absb, alb, cosz[None], ext, ssa, asy, gas[None], sol[None], band[None])


def column_features(aerosol_mass, size_bins, bin_count):
    mode_count, levels, total_cols = aerosol_mass.shape
    first = (jnp.log(aerosol_mass) + 4.6) / 1.4
    second = (size_bins.astype(jnp.float32) - bin_count / 2) / (bin_count / 2)
    stacked = jnp.concatenate(
        [
            first.reshape(mode_count * levels, total_cols),
            second.reshape(mode_count * levels, total_cols),
        ],
        axis=0,
    )
    return stacked.astype(jnp.bfloat16)


def learner_terms(slot_rows, slot_goals, slot_valid, w_full, b_full, w_head, loss_scale):
    pre_act = (
        jnp.dot(slot_rows, w_full.T, preferred_element_type=jnp.float32)
        + b_full.astype(jnp.float32)[None, :]
    )
    active, slope = jax.vjp(partial(jax.nn.gelu, approximate=True), pre_act)
    hidden = active.astype(jnp.bfloat16)
    predicted = jnp.dot(hidden, w_head, preferred_element_type=jnp.float32)
    error_rows = (predicted - slot_goals.astype(jnp.float32)) * slot_valid.astype(jnp.float32)[
        :, None
    ]
    pred_grad = (error_rows * loss_scale).astype(jnp.bfloat16)
    hidden_grad = jnp.dot(pred_grad, w_head.T, preferred_element_type=jnp.float32)
    pre_grad = slope(hidden_grad)[0].astype(jnp.bfloat16)
    trunk_part = jnp.dot(pre_grad.T, slot_rows, preferred_element_type=jnp.float32)
    bias_part = jnp.sum(pre_grad, axis=0, dtype=jnp.float32)
    return (hidden, pred_grad, trunk_part, bias_part)


def per_device(
    aerosol_mass,
    size_bins,
    cloud_tau,
    cloud_mask,
    absorber,
    surface_albedo,
    cos_zenith,
    ext_table,
    ssa_table,
    asym_table,
    gas_coeff,
    solar_flux,
    band_map,
    column_learner,
    trunk_weight,
    trunk_bias,
    head_weight,
):
    fluxes = evolve(
        aerosol_mass,
        size_bins,
        cloud_tau,
        cloud_mask,
        absorber,
        surface_albedo,
        cos_zenith,
        ext_table,
        ssa_table,
        asym_table,
        gas_coeff,
        solar_flux,
        band_map,
    )
    features = column_features(
        aerosol_mass, size_bins, BINS
    )
    targets = fluxes.astype(jnp.bfloat16)
    columns_here = aerosol_mass.shape[-1]
    learners = lax.axis_size(LRN)
    capacity = 2 * columns_here // learners
    slot_count = learners * capacity
    destination = column_learner[:, 0]
    dest_hot = (destination[:, None] == jnp.arange(learners, dtype=jnp.int32)[None, :]).astype(
        jnp.int32
    )
    slot_rank = jnp.sum((jnp.cumsum(dest_hot, axis=0) - dest_hot) * dest_hot, axis=1)
    slot_index = destination * capacity + slot_rank
    dispatch = (jnp.arange(slot_count, dtype=jnp.int32)[:, None] == slot_index[None, :]).astype(
        jnp.bfloat16
    )
    packed = jnp.concatenate([features, targets], axis=0)
    slot_data = jnp.dot(dispatch, packed.T, preferred_element_type=jnp.float32).astype(jnp.bfloat16)
    feature_width = features.shape[0]
    row_feat = slot_data[:, :feature_width]
    row_goal = slot_data[:, feature_width:]
    filled = jnp.sum(dispatch, axis=1, dtype=jnp.float32).astype(jnp.bfloat16)
    slot_rows, slot_goals, slot_valid = in_one_piece((row_feat, row_goal, filled), LRN, 0, 0, 1)
    w_full, b_full = in_one_piece_2((trunk_weight, trunk_bias), ("lrn_0", ("lrn_1", "lrn_2")), 0, 1)
    hidden, pred_grad, trunk_part, bias_part = learner_terms(
        slot_rows, slot_goals, slot_valid, w_full, b_full, head_weight[0], 1.0 / COL_DEV
    )
    head_local = jnp.dot(hidden.T, pred_grad, preferred_element_type=jnp.float32)
    head_part = sent_and_summed(head_local, "grp", 0)
    head_sum = collect(head_part, "grp", 0)
    share_w, share_b = in_one_piece_3(
        (trunk_part.astype(jnp.bfloat16), bias_part.astype(jnp.bfloat16)),
        ("lrn_0", ("lrn_1", "lrn_2")),
        0,
        1,
    )
    trunk_grad, bias_grad = packed_total((share_w, share_b), "grp")
    return (fluxes, head_sum[None], trunk_grad, bias_grad)


def solution(mesh):
    split = Mesh(
        mesh.devices.reshape(mesh.shape["grp"], 4, 4, 8), ("grp", "lrn_0", "lrn_1", "lrn_2")
    )
    placed = (
        P(None, None, GRP_LRN),
        P(None, None, GRP_LRN),
        P(None, GRP_LRN),
        P(GRP_LRN),
        P(None, GRP_LRN),
        P(None, GRP_LRN),
        P(GRP_LRN),
        P(),
        P(),
        P(),
        P(),
        P(),
        P(),
        P(GRP_LRN, None),
        P(LRN, None),
        P(LRN),
        P(LRN, None, None),
    )
    return jax.shard_map(
        per_device,
        mesh=split,
        in_specs=placed,
        out_specs=(P(None, GRP_LRN), P(LRN, None, None), P(LRN, None), P(LRN)),
        check_vma=False,
    )
```

```python
import math

import jax
import jax.numpy as jnp
from jax import lax
from jax.experimental import pallas as pl
from jax.experimental.pallas import tpu as pltpu
from jax.sharding import Mesh
from jax.sharding import PartitionSpec as P

MODES = 4
BINS = 64
G = 112
NB = 14
LEV = 32
COL_DEV = 128
LRN = ("x", "zl", "y")
GRP_LRN = ("zh", "cc", "x", "zl", "y")
MESH = pl.DeviceIdType.MESH
BF = jnp.bfloat16
F32 = jnp.float32
CLOUD_SSA = 0.99
CLOUD_ASYM = 0.85


def nt(a, b):
    return lax.dot_general(a, b, (((1,), (1,)), ((), ())), preferred_element_type=F32)


def nn(a, b):
    return jnp.dot(a, b, preferred_element_type=F32)


def iota(shape, dim):
    return lax.broadcasted_iota(jnp.int32, shape, dim)


def row_to_col(row):
    n = row.shape[1]
    rows = lax.broadcasted_iota(jnp.int32, (n, n), 0)
    cols = lax.broadcasted_iota(jnp.int32, (n, n), 1)
    return jnp.sum(jnp.where(rows == cols, jnp.broadcast_to(row, (n, n)), 0.0), axis=1, keepdims=True)


def evolve_setup(ext, ssa, asy, gas, sol, band, tab, gcol, m0):
    e = ext[...]
    s = e * ssa[...]
    tab[0:G, :] = e.astype(jnp.bfloat16)
    tab[G : 2 * G, :] = s.astype(jnp.bfloat16)
    tab[2 * G : 3 * G, :] = (s * asy[...]).astype(jnp.bfloat16)
    gcol[...] = jnp.broadcast_to(row_to_col(gas[...]), (G, COL_DEV))
    bcol = row_to_col(band[...].astype(jnp.float32))
    m0[...] = jnp.broadcast_to(jnp.where(bcol < NB // 2, 1.0, 0.0), (G, COL_DEV))
    return bcol


CH = 8
LU = 4


def evolve_layers(mass, bins, tau, mask, absb, tab, gcol, opt, refl, trans):
    labels = lax.broadcasted_iota(jnp.int32, (BINS, COL_DEV), 0)
    cloudy_on = mask[...].astype(jnp.float32)

    def body(step, carry):
        pieces = []
        for u in range(LU):
            l = step * LU + u
            modes = []
            for m in range(MODES):
                load = mass[m, pl.ds(l, 1), :]
                hot = bins[m, pl.ds(l, 1), :] == labels
                modes.append(jnp.where(hot, jnp.broadcast_to(load, (BINS, COL_DEV)), 0.0))
            pieces.append(jnp.concatenate(modes, axis=0).astype(jnp.bfloat16))
        weights = jnp.concatenate(pieces, axis=1)
        opt[...] = jnp.dot(tab[...], weights, preferred_element_type=jnp.float32)
        for u in range(LU):
            l = step * LU + u
            cl = tau[pl.ds(l, 1), :] * cloudy_on
            ab = absb[pl.ds(l, 1), :]
            c1 = CLOUD_SSA * cl
            c2 = CLOUD_SSA * CLOUD_ASYM * cl
            lanes = slice(u * COL_DEV, (u + 1) * COL_DEV)
            for g in range(0, G, CH):
                d = opt[g : g + CH, lanes] + cl + gcol[g : g + CH, :] * ab
                s = opt[G + g : G + g + CH, lanes] + c1
                f = opt[2 * G + g : 2 * G + g + CH, lanes] + c2
                ds, df = d - s, d - f
                k = 2.0 * jnp.sqrt(ds * df)
                g1 = ds + df
                e = jnp.exp(-k)
                sq = e * e
                r = 1.0 / ((k + g1) + (k - g1) * sq)
                refl[l, g : g + CH, :] = (s - f) * (1.0 - sq) * r
                trans[l, g : g + CH, :] = 2.0 * k * e * r
        return carry

    lax.fori_loop(0, LEV // LU, body, 0)


def evolve_up(alb, bcol, refl, trans, below):
    surface = jnp.zeros((G, COL_DEV), jnp.float32)
    for b in range(NB):
        surface = jnp.where(bcol == float(b), jnp.broadcast_to(alb[b : b + 1, :], (G, COL_DEV)), surface)
    below[LEV] = surface

    def body(step, carry):
        l = LEV - 1 - step
        for g in range(0, G, CH):
            rows = slice(g, g + CH)
            b = below[l + 1, rows, :]
            r = refl[l, rows, :]
            t = trans[l, rows, :]
            q = t / (1.0 - r * b)
            below[l, rows, :] = r + t * b * q
            trans[l, rows, :] = q
        return carry

    lax.fori_loop(0, LEV, body, 0)


def evolve_down(sol, cosz, m0, below, trans, down, flux):
    cosv = cosz[...]
    scol = row_to_col(sol[...])
    down[...] = jnp.broadcast_to(scol, (G, COL_DEV)) * cosv
    scale = 2.0 / G

    def body(l, carry):
        acc = [jnp.zeros((CH, COL_DEV), jnp.float32) for _ in range(4)]
        for g in range(0, G, CH):
            rows = slice(g, g + CH)
            now = down[rows, :]
            low = m0[rows, :]
            up = below[l, rows, :] * now
            nxt = trans[l, rows, :] * now
            down[rows, :] = nxt
            nl, ul = nxt * low, up * low
            acc[0] = acc[0] + nl
            acc[1] = acc[1] + ul
            acc[2] = acc[2] + (nxt - nl)
            acc[3] = acc[3] + (up - ul)
        for i in range(4):
            flux[pl.ds(i * LEV + l, 1), :] = jnp.sum(acc[i], axis=0, keepdims=True) * scale
        return carry

    lax.fori_loop(0, LEV, body, 0)


EMPTY = 2.0
ROOT = math.sqrt(2.0 / math.pi)
CUBE = 0.044715


def remote(src, dst, send, recv, **at):
    return pltpu.make_async_remote_copy(
        src_ref=src, dst_ref=dst, send_sem=send, recv_sem=recv, device_id=at, device_id_type=MESH
    )


def wait_bytes(ref, sem):
    pltpu.make_async_copy(ref, ref, sem).wait()


def send_features(mass, bins, lr, fs, slot_col):
    row = lr[...]
    col = row_to_col(row.astype(F32))
    same = jnp.broadcast_to(col, (COL_DEV, COL_DEV)) == jnp.broadcast_to(row.astype(F32), (COL_DEV, COL_DEV))
    before = iota((COL_DEV, COL_DEV), 0) < iota((COL_DEV, COL_DEV), 1)
    rank = jnp.sum(jnp.where(same & before, 1.0, 0.0), axis=0, keepdims=True).astype(jnp.int32)
    peer = (row >> 5) * 8 + (row & 7)
    key = peer * 16 + ((row >> 3) & 3) * 4 + rank
    slot_col[...] = peer * 8 + ((row >> 3) & 3) * 2 + rank
    first = ((jnp.log(mass[...]) + 4.6) / 1.4).reshape(MODES * LEV, COL_DEV).astype(BF)
    half = BINS / 2
    second = ((bins[...].astype(F32) - half) / half).reshape(MODES * LEV, COL_DEV).astype(BF)
    rows = iota((512, COL_DEV), 0)
    hot0 = jnp.where(rows == key, 1.0, 0.0).astype(BF)
    hot1 = jnp.where(rows == key + 2, 1.0, 0.0).astype(BF)
    data = nt(hot0, first) + nt(hot1, second)
    filled = nn(hot0 + hot1, jnp.ones((COL_DEV, COL_DEV), BF))
    empty = (filled < 0.5) & (iota((512, COL_DEV), 1) == 0)
    fs[...] = jnp.where(empty, EMPTY, data).reshape(32, 16, COL_DEV).astype(BF)


def kernel(
    mass, bins, tau, mask, absb, alb, cosz, ext, ssa, asy, gas, sol, band, lr, w, b, hw,
    flux, head, tg, bg,
    tab, gcol, m0, opt, refl, trans, below, down,
    slot_col, fs, fr, fz, fx, fo, ts, tr, tz, tx, to, wz, bs, br, bz, hv, hwt, biasc,
    xs, pre, slope, ht, pp, po, gt, ta, tps, bps, tpr, bpr, fsum, fbsum, gr, gb, hg,
    s_w, r_w, s_b, r_b, s_f, r_f, s_wz, r_wz, s_bz, r_bz, s_fz, r_fz, s_fd, r_fd,
    s_t, r_t, s_tz, r_tz, s_td, r_td, s_p, r_p, s_h, r_h, l_h, l_hw,
    s_k, r_k, s_kb, r_kb, s_e, r_e, s_eb, r_eb,
):
    zh, cc, x, zl, y = (lax.axis_index(a) for a in GRP_LRN)
    other = 1 - cc
    me = x * 8 + y
    z = zh * 4 + zl
    part = 2 * cc + zh
    own_piece = (part == x) & (x == zl)

    def plane(i):
        p = lax.rem(me + i, 32)
        return p, lax.div(p, 8), lax.rem(p, 8)

    def ring(i):
        q = lax.rem(z + i, 8)
        return lax.div(q, 4), lax.rem(q, 4)

    barrier = pltpu.get_barrier_semaphore()

    def greet(i, c):
        _, px, py = plane(i)
        pl.semaphore_signal(barrier, inc=1, device_id={"x": px, "y": py}, device_id_type=MESH)
        return c

    lax.fori_loop(1, 32, greet, 0)
    for i in range(1, 8):
        qh, ql = ring(i)
        pl.semaphore_signal(barrier, inc=1, device_id={"zh": qh, "zl": ql}, device_id_type=MESH)
    pl.semaphore_signal(barrier, inc=1, device_id={"cc": other}, device_id_type=MESH)
    for a in range(4):

        @pl.when(jnp.logical_not(own_piece & (zl == a)))
        def _():
            at = {"zh": lax.rem(x, 2), "cc": lax.div(x, 2), "x": zl, "zl": a}
            pl.semaphore_signal(barrier, inc=1, device_id=at, device_id_type=MESH)

    hw_copy = pltpu.make_async_copy(hw.at[pl.ds(2 * cc, 2)], hv, l_hw)
    hw_copy.start()

    send_features(mass, bins, lr, fs, slot_col)
    spread = (iota((16, COL_DEV), 1) == y * 16 + iota((16, COL_DEV), 0)).astype(BF)
    bs[...] = nn(b[...], spread)
    sender = lax.div(x, 2) == cc
    xb = lax.rem(x, 2)

    @pl.when(own_piece)
    def _():
        pl.semaphore_wait(barrier, 42)

    @pl.when(jnp.logical_not(own_piece))
    def _():
        pl.semaphore_wait(barrier, 43)

    @pl.when(sender)
    def _():
        def go(i, c):
            _, px, py = plane(i)
            remote(w, wz.at[xb, zl, y], s_w, r_w, x=px, y=py).start()
            remote(bs, br.at[xb, y], s_b, r_b, x=px, y=py).start()
            return c

        lax.fori_loop(1, 32, go, 0)
        wz[xb, zl, y] = w[...]
        br[xb, y] = bs[...]

    def go_features(i, c):
        p, px, py = plane(i)
        remote(fs.at[p], fr.at[me], s_f, r_f, x=px, y=py).start()
        return c

    lax.fori_loop(1, 32, go_features, 0)
    fr[me] = fs[me]

    bcol = evolve_setup(ext, ssa, asy, gas, sol, band, tab, gcol, m0)
    evolve_layers(mass, bins, tau, mask, absb, tab, gcol, opt, refl, trans)

    @pl.when(sender)
    def _():
        wait_bytes(tpr.at[0:15], r_w)
        wait_bytes(bpr.at[0:15], r_b)

    @pl.when(jnp.logical_not(sender))
    def _():
        wait_bytes(tpr.at[0:16], r_w)
        wait_bytes(bpr.at[0:16], r_b)

    for a in range(2):
        bz[a, zl] = jnp.sum(br[a], axis=0)
    for step in (1, 7, 2 + 4 * cc):
        qh, ql = ring(step)
        remote(wz.at[:, zl], wz.at[:, zl], s_wz, r_wz, zh=qh, zl=ql).start()
        remote(bz.at[:, zl], bz.at[:, zl], s_bz, r_bz, zh=qh, zl=ql).start()

    wait_bytes(fr.at[0:31], r_f)
    got = fr[...].reshape(512, COL_DEV)
    o = iota((COL_DEV, 512), 0)
    source = ((o >> 1) & 31) * 16 + (o >> 6) * 2 + (o & 1)
    shift = iota((COL_DEV, 512), 1) - source
    for a in range(4):
        pick = jnp.where(shift == 4 * a, 1.0, 0.0).astype(BF)
        fz[a] = nn(pick, got).astype(BF)
    for i in (4, 3, 5, 2, 6, 1, 7):
        qh, ql = ring(i)
        remote(fz.at[ql], fx.at[z], s_fz, r_fz, zh=qh, zl=ql).start()
    fx[z] = fz[zl]

    evolve_up(alb, bcol, refl, trans, below)
    evolve_down(sol, cosz, m0, below, trans, down, flux)

    place = jnp.where(iota((256, COL_DEV), 0) == slot_col[...], 1.0, 0.0).astype(BF)
    ts[...] = nt(place, flux[...].astype(BF)).reshape(32, 8, COL_DEV).astype(BF)

    def go_targets(i, c):
        p, px, py = plane(i)
        remote(ts.at[p], tr.at[me], s_t, r_t, x=px, y=py).start()
        return c

    lax.fori_loop(1, 32, go_targets, 0)
    tr[me] = ts[me]

    hw_copy.wait()
    eye = jnp.where(iota((COL_DEV, COL_DEV), 0) == iota((COL_DEV, COL_DEV), 1), 1.0, 0.0).astype(BF)
    for a in range(2):
        hwt[a] = nt(eye, hv[a]).astype(BF)
    wait_bytes(fx.at[0:7], r_fz)
    fd = remote(fx, fo, s_fd, r_fd, cc=other)
    fd.start()
    wait_bytes(bz.at[:, 0:3], r_bz)
    for a in range(2):
        for q in range(4):
            biasc[a, q * COL_DEV : (q + 1) * COL_DEV, :] = jnp.broadcast_to(row_to_col(bz[a, q]), (COL_DEV, COL_DEV))
    wait_bytes(wz.at[:, 0:3], r_wz)

    def gather_x(side, ref):
        for q in range(8):
            for h in range(2):
                xs[side * 2 + q // 4, (q % 4) * 64 : (q % 4 + 1) * 64, h * COL_DEV : (h + 1) * COL_DEV] = ref[
                    q, h * 64 : (h + 1) * 64, :
                ]

    gather_x(0, fx)

    def forward(sb, half, with_slope):
        pre[...] = nt(wz[half].reshape(512, 256), xs[sb])
        for r in range(0, 512, 32):
            v = pre[r : r + 32, :]
            bc = biasc[half, r : r + 32, :]
            v = v + jnp.concatenate([bc, bc], axis=1)
            sq = v * v
            t = jnp.tanh(ROOT * (v + CUBE * (v * sq)))
            cdf = 0.5 + 0.5 * t
            ht[sb, half, r : r + 32, :] = (v * cdf).astype(BF)
            if with_slope:
                slope[sb, r : r + 32, :] = cdf + (0.5 * v) * ((1.0 - t * t) * (ROOT + (3.0 * CUBE * ROOT) * sq))
        return nn(hwt[half], ht[sb, half])

    def forward_block(sb, c):
        pp[sb] = forward(sb, zh, True) + forward(sb, 1 - zh, False)
        return c

    lax.fori_loop(0, 2, forward_block, 0)

    wait_bytes(tr.at[0:31], r_t)
    gott = tr[...].astype(F32).reshape(256, COL_DEV).astype(BF)
    ot = iota((64, 256), 0)
    shift_t = iota((64, 256), 1) - ((ot >> 1) * 8 + (ot & 1))
    for a in range(4):
        tz[a] = nn(jnp.where(shift_t == 2 * a, 1.0, 0.0).astype(BF), gott).astype(BF)
    for i in (4, 3, 5, 2, 6, 1, 7):
        qh, ql = ring(i)
        remote(tz.at[ql], tx.at[z], s_tz, r_tz, zh=qh, zl=ql).start()
    tx[z] = tz[zl]

    fd.wait()
    gather_x(1, fo)
    lax.fori_loop(2, 4, forward_block, 0)
    pd = remote(pp, po, s_p, r_p, cc=other)
    pd.start()

    wait_bytes(tx.at[0:7], r_tz)
    td = remote(tx, to, s_td, r_td, cc=other)
    td.start()
    pd.wait()
    td.wait()
    lane0 = jnp.where(iota((8, COL_DEV), 1) == 0, 1.0, 0.0).astype(BF)
    for sb in range(4):
        src = (tx, tx, to, to)[sb]
        goal = nt(eye, src[(sb % 2) * 4 : (sb % 2) * 4 + 4].reshape(256, COL_DEV))
        flag = nt(lane0, xs[sb, :, COL_DEV:])[0:1, :]
        factor = jnp.where(flag < 1.5, 1.0 / COL_DEV, 0.0)
        gt[sb] = (((pp[sb] + po[(sb + 2) % 4]) - goal) * factor).astype(BF)

    ones = jnp.ones((8, 256), BF)
    ta[...] = jnp.zeros_like(ta)

    def backward(sb, brow):
        hgrad = nn(hv[zh], gt[sb])
        pgrad = (hgrad * slope[sb]).astype(BF)
        ta[...] += nn(pgrad, xs[sb])
        return brow + nt(ones, pgrad)

    brow = lax.fori_loop(0, 4, backward, jnp.zeros((8, 512), F32))
    tps[...] = ta[...].reshape(32, 16, 256).astype(BF)
    for a in range(4):
        bps[a] = brow[0:1, a * COL_DEV : (a + 1) * COL_DEV]

    def go_trunk(i, c):
        p, px, py = plane(i)
        remote(tps.at[p], tpr.at[me], s_k, r_k, x=px, y=py).start()
        remote(bps.at[px], bpr.at[me], s_kb, r_kb, x=px, y=py).start()
        return c

    lax.fori_loop(1, 32, go_trunk, 0)
    tpr[me] = tps[me]
    bpr[me] = bps[x]

    for half in range(2):
        total = nt(ht[0, half], gt[0])
        for sb in range(1, 4):
            total = total + nt(ht[sb, half], gt[sb])
        hg[half] = total
    hd = remote(hg, head.at[pl.ds(2 * cc, 2)], s_h, r_h, cc=other)
    hd.start()
    hl = pltpu.make_async_copy(hg, head.at[pl.ds(2 * cc, 2)], l_h)
    hl.start()

    wait_bytes(tpr.at[0:31], r_k)
    wait_bytes(bpr.at[0:31], r_kb)
    fsum[...] = jnp.sum(tpr[...].astype(F32), axis=0)
    fbsum[...] = jnp.sum(bpr[...], axis=0)
    for qh in range(2):
        for qc in range(2):
            mine = own_piece & (zh == qh) & (cc == qc)

            @pl.when(jnp.logical_not(mine))
            def _():
                at = dict(zh=qh, cc=qc, x=part, zl=x)
                remote(fsum, gr.at[zl], s_e, r_e, **at).start()
                remote(fbsum, gb.at[zl], s_eb, r_eb, **at).start()

            @pl.when(mine)
            def _():
                gr[zl] = fsum[...]
                gb[zl] = fbsum[...]

    @pl.when(own_piece)
    def _():
        wait_bytes(gr.at[0:3], r_e)
        wait_bytes(gb.at[0:3], r_eb)

    @pl.when(jnp.logical_not(own_piece))
    def _():
        wait_bytes(gr, r_e)
        wait_bytes(gb, r_eb)

    tg[...] = (gr[0] + gr[1]) + (gr[2] + gr[3])
    brows = (gb[0] + gb[1]) + (gb[2] + gb[3])
    kept = jnp.where(lax.div(iota((1, COL_DEV), 1), 16) == y, brows, 0.0)
    bias = kept[:, 0:16]
    for a in range(1, 8):
        bias = bias + kept[:, a * 16 : (a + 1) * 16]
    bg[...] = bias

    hl.wait()
    hd.wait_send()
    wait_bytes(head.at[pl.ds(2 * other, 2)], r_h)

    @pl.when(sender)
    def _():
        wait_bytes(tpr.at[0:31], s_w)
        wait_bytes(bpr.at[0:31], s_b)

    wait_bytes(fs.at[0:31], s_f)
    wait_bytes(wz.at[:, 0:3], s_wz)
    wait_bytes(bz.at[:, 0:3], s_bz)
    wait_bytes(fx.at[0:7], s_fz)
    wait_bytes(ts.at[0:31], s_t)
    wait_bytes(tx.at[0:7], s_tz)
    wait_bytes(tps.at[0:31], s_k)
    wait_bytes(bpr.at[0:31], s_kb)

    @pl.when(own_piece)
    def _():
        wait_bytes(gr.at[0:3], s_e)
        wait_bytes(gb.at[0:3], s_eb)

    @pl.when(jnp.logical_not(own_piece))
    def _():
        wait_bytes(gr, s_e)
        wait_bytes(gb, s_eb)


def per_device(mass, bins, tau, mask, absb, alb, cosz, ext, ssa, asy, gas, sol, band, lr, w, b, hw):
    vm = pl.BlockSpec(memory_space=pltpu.VMEM)
    hbm = pl.BlockSpec(memory_space=pl.ANY)
    v = pltpu.VMEM
    c = COL_DEV
    flux, head, tg, bg = pl.pallas_call(
        kernel,
        out_shape=(
            jax.ShapeDtypeStruct((4 * LEV, c), F32),
            jax.ShapeDtypeStruct((4, 512, c), F32),
            jax.ShapeDtypeStruct((16, 256), F32),
            jax.ShapeDtypeStruct((1, 16), F32),
        ),
        in_specs=[vm] * 16 + [hbm],
        out_specs=(vm, hbm, vm, vm),
        scratch_shapes=[
            v((3 * G, MODES * BINS), BF), v((G, c), F32), v((G, c), F32), v((3 * G, LU * c), F32),
            v((LEV, G, c), F32), v((LEV, G, c), F32), v((LEV + 1, G, c), F32), v((G, c), F32),
            v((1, c), jnp.int32),
            v((32, 16, c), BF), v((32, 16, c), BF), v((4, 128, c), BF), v((8, 128, c), BF), v((8, 128, c), BF),
            v((32, 8, c), BF), v((32, 8, c), BF), v((4, 64, c), BF), v((8, 64, c), BF), v((8, 64, c), BF),
            v((2, 4, 8, 16, 256), BF), v((1, c), F32), v((2, 8, 1, c), F32), v((2, 4, 1, c), F32),
            v((2, 512, c), BF), v((2, c, 512), BF), v((2, 512, c), F32),
            v((4, 256, 256), BF), v((512, 256), F32), v((4, 512, 256), F32), v((4, 2, 512, 256), BF),
            v((4, c, 256), F32), v((4, c, 256), F32), v((4, c, 256), BF), v((512, 256), F32),
            v((32, 16, 256), BF), v((4, 1, c), F32), v((32, 16, 256), BF), v((32, 1, c), F32),
            v((16, 256), F32), v((1, c), F32), v((4, 16, 256), F32), v((4, 1, c), F32), v((2, 512, c), F32),
        ] + [pltpu.SemaphoreType.DMA] * 34,
        compiler_params=pltpu.CompilerParams(collective_id=0, has_side_effects=True),
    )(
        mass, bins, tau, mask[None], absb, alb, cosz[None], ext, ssa, asy, gas[None], sol[None], band[None],
        lr.reshape(1, c), w, b[None], hw.reshape(4, 512, c),
    )
    return flux, head.reshape(1, 2048, c), tg, bg[0]


def solution(mesh):
    split = Mesh(mesh.devices.reshape(2, 2, 4, 4, 8), GRP_LRN)
    placed = (
        P(None, None, GRP_LRN),
        P(None, None, GRP_LRN),
        P(None, GRP_LRN),
        P(GRP_LRN),
        P(None, GRP_LRN),
        P(None, GRP_LRN),
        P(GRP_LRN),
        P(),
        P(),
        P(),
        P(),
        P(),
        P(),
        P(GRP_LRN, None),
        P(LRN, None),
        P(LRN),
        P(LRN, None, None),
    )
    return jax.shard_map(
        per_device,
        mesh=split,
        in_specs=placed,
        out_specs=(P(None, GRP_LRN), P(LRN, None, None), P(LRN, None), P(LRN)),
        check_vma=False,
    )
```

```python
import math

import jax
import jax.numpy as jnp
from jax import lax
from jax.experimental import pallas as pl
from jax.experimental.pallas import tpu as pltpu
from jax.sharding import Mesh
from jax.sharding import PartitionSpec as P

MODES = 4
BINS = 64
G = 112
NB = 14
LEV = 32
COL_DEV = 128
LRN = ("x", "zl", "y")
GRP_LRN = ("zh", "cc", "x", "zl", "y")
MESH = pl.DeviceIdType.MESH
BF = jnp.bfloat16
F32 = jnp.float32
CLOUD_SSA = 0.99
CLOUD_ASYM = 0.85


def nt(a, b):
    return lax.dot_general(a, b, (((1,), (1,)), ((), ())), preferred_element_type=F32)


def nn(a, b):
    return jnp.dot(a, b, preferred_element_type=F32)


def iota(shape, dim):
    return lax.broadcasted_iota(jnp.int32, shape, dim)


def row_to_col(row):
    n = row.shape[1]
    rows = lax.broadcasted_iota(jnp.int32, (n, n), 0)
    cols = lax.broadcasted_iota(jnp.int32, (n, n), 1)
    return jnp.sum(jnp.where(rows == cols, jnp.broadcast_to(row, (n, n)), 0.0), axis=1, keepdims=True)


def evolve_setup(ext, ssa, asy, gas, sol, band, tab, gcol, m0):
    e = ext[...]
    s = e * ssa[...]
    tab[0:G, :] = e.astype(jnp.bfloat16)
    tab[G : 2 * G, :] = s.astype(jnp.bfloat16)
    tab[2 * G : 3 * G, :] = (s * asy[...]).astype(jnp.bfloat16)
    gcol[...] = jnp.broadcast_to(row_to_col(gas[...]), (G, COL_DEV))
    bcol = row_to_col(band[...].astype(jnp.float32))
    m0[...] = jnp.broadcast_to(jnp.where(bcol < NB // 2, 1.0, 0.0), (G, COL_DEV))
    return bcol


CH = 8
LU = 4


def evolve_layers(mass, bins, tau, mask, absb, tab, gcol, opt, refl, trans):
    labels = lax.broadcasted_iota(jnp.int32, (BINS, COL_DEV), 0)
    cloudy_on = mask[...].astype(jnp.float32)

    def body(step, carry):
        pieces = []
        for u in range(LU):
            l = step * LU + u
            modes = []
            for m in range(MODES):
                load = mass[m, pl.ds(l, 1), :]
                hot = bins[m, pl.ds(l, 1), :] == labels
                modes.append(jnp.where(hot, jnp.broadcast_to(load, (BINS, COL_DEV)), 0.0))
            pieces.append(jnp.concatenate(modes, axis=0).astype(jnp.bfloat16))
        weights = jnp.concatenate(pieces, axis=1)
        opt[...] = jnp.dot(tab[...], weights, preferred_element_type=jnp.float32)
        for u in range(LU):
            l = step * LU + u
            cl = tau[pl.ds(l, 1), :] * cloudy_on
            ab = absb[pl.ds(l, 1), :]
            c1 = CLOUD_SSA * cl
            c2 = CLOUD_SSA * CLOUD_ASYM * cl
            lanes = slice(u * COL_DEV, (u + 1) * COL_DEV)
            for g in range(0, G, CH):
                d = opt[g : g + CH, lanes] + cl + gcol[g : g + CH, :] * ab
                s = opt[G + g : G + g + CH, lanes] + c1
                f = opt[2 * G + g : 2 * G + g + CH, lanes] + c2
                ds, df = d - s, d - f
                k = 2.0 * jnp.sqrt(ds * df)
                g1 = ds + df
                e = jnp.exp(-k)
                sq = e * e
                r = 1.0 / ((k + g1) + (k - g1) * sq)
                refl[l, g : g + CH, :] = (s - f) * (1.0 - sq) * r
                trans[l, g : g + CH, :] = 2.0 * k * e * r
        return carry

    lax.fori_loop(0, LEV // LU, body, 0)


def evolve_up(alb, bcol, refl, trans, below):
    surface = jnp.zeros((G, COL_DEV), jnp.float32)
    for b in range(NB):
        surface = jnp.where(bcol == float(b), jnp.broadcast_to(alb[b : b + 1, :], (G, COL_DEV)), surface)
    below[LEV] = surface

    def body(step, carry):
        l = LEV - 1 - step
        layer = [(refl[l, g : g + CH, :], trans[l, g : g + CH, :]) for g in range(0, G, CH)]
        nxt, ratio = [], []
        for b, (r, t) in zip(carry, layer):
            q = t / (1.0 - r * b)
            ratio.append(q)
            nxt.append(r + t * b * q)
        for i, g in enumerate(range(0, G, CH)):
            below[l, g : g + CH, :] = nxt[i]
            trans[l, g : g + CH, :] = ratio[i]
        return tuple(nxt)

    lax.fori_loop(0, LEV, body, tuple(surface[g : g + CH, :] for g in range(0, G, CH)))


def evolve_down(sol, cosz, m0, below, trans, down, flux):
    cosv = cosz[...]
    scol = row_to_col(sol[...])
    down[...] = jnp.broadcast_to(scol, (G, COL_DEV)) * cosv
    scale = 2.0 / G

    def body(l, carry):
        acc = [jnp.zeros((CH, COL_DEV), jnp.float32) for _ in range(4)]
        for g in range(0, G, CH):
            rows = slice(g, g + CH)
            now = down[rows, :]
            low = m0[rows, :]
            up = below[l, rows, :] * now
            nxt = trans[l, rows, :] * now
            down[rows, :] = nxt
            nl, ul = nxt * low, up * low
            acc[0] = acc[0] + nl
            acc[1] = acc[1] + ul
            acc[2] = acc[2] + (nxt - nl)
            acc[3] = acc[3] + (up - ul)
        for i in range(4):
            flux[pl.ds(i * LEV + l, 1), :] = jnp.sum(acc[i], axis=0, keepdims=True) * scale
        return carry

    lax.fori_loop(0, LEV, body, 0)


EMPTY = 2.0
ROOT = math.sqrt(2.0 / math.pi)
CUBE = 0.044715


def remote(src, dst, send, recv, **at):
    return pltpu.make_async_remote_copy(
        src_ref=src, dst_ref=dst, send_sem=send, recv_sem=recv, device_id=at, device_id_type=MESH
    )


def wait_bytes(ref, sem):
    pltpu.make_async_copy(ref, ref, sem).wait()


def send_features(mass, bins, lr, fs, slot_col):
    row = lr[...]
    col = row_to_col(row.astype(F32))
    same = jnp.broadcast_to(col, (COL_DEV, COL_DEV)) == jnp.broadcast_to(row.astype(F32), (COL_DEV, COL_DEV))
    before = iota((COL_DEV, COL_DEV), 0) < iota((COL_DEV, COL_DEV), 1)
    rank = jnp.sum(jnp.where(same & before, 1.0, 0.0), axis=0, keepdims=True).astype(jnp.int32)
    peer = (row >> 5) * 8 + (row & 7)
    key = peer * 16 + ((row >> 3) & 3) * 4 + rank
    slot_col[...] = peer * 8 + ((row >> 3) & 3) * 2 + rank
    first = ((jnp.log(mass[...]) + 4.6) / 1.4).reshape(MODES * LEV, COL_DEV).astype(BF)
    half = BINS / 2
    second = ((bins[...].astype(F32) - half) / half).reshape(MODES * LEV, COL_DEV).astype(BF)
    rows = iota((512, COL_DEV), 0)
    hot0 = jnp.where(rows == key, 1.0, 0.0).astype(BF)
    hot1 = jnp.where(rows == key + 2, 1.0, 0.0).astype(BF)
    data = nt(hot0, first) + nt(hot1, second)
    filled = nn(hot0 + hot1, jnp.ones((COL_DEV, COL_DEV), BF))
    empty = (filled < 0.5) & (iota((512, COL_DEV), 1) == 0)
    fs[...] = jnp.where(empty, EMPTY, data).reshape(32, 16, COL_DEV).astype(BF)


def kernel(
    mass_in, bins_in, tau_in, mask_in, absb_in, alb_in, cosz_in, ext_in, ssa_in, asy_in, gas_in, sol_in, band_in,
    lr_in, w_in, b_in, hw,
    flux, head, tg, bg,
    mass, bins, tau, mask, absb, alb, cosz, ext, ssa, asy, gas, sol, band, lr, w, b, in_sems,
    tab, gcol, m0, opt, refl, trans, below, down,
    slot_col, fs, fr, fz, fx, fo, ts, tr, tz, tx, to, wa, wb, wl, bs, br, bz, hv, hwt, biasc,
    xs, pre, slope, ht, pp, po, gt, ta, tps, bps, tpr, bpr, fsum, fbsum, gr, gb, hg,
    s_w, r_w, s_b, r_b, s_f, r_f, s_wz, r_wz, s_bz, r_bz, s_wl, r_wl, s_wy, r_wy, s_wx, r_wx, s_fz, r_fz, s_fd, r_fd,
    s_t, r_t, s_tz, r_tz, s_td, r_td, s_p, r_p, s_p1, r_p1, s_h, r_h, l_h, l_hw,
    s_k, r_k, s_kb, r_kb, s_e, r_e, s_eb, r_eb,
):
    zh, cc, x, zl, y = (lax.axis_index(a) for a in GRP_LRN)
    other = 1 - cc
    me = x * 8 + y
    z = zh * 4 + zl
    part = 2 * cc + zh
    own_piece = (part == x) & (x == zl)

    def plane(i):
        p = lax.rem(me + i, 32)
        return p, lax.div(p, 8), lax.rem(p, 8)

    def ring(i):
        q = lax.rem(z + i, 8)
        return lax.div(q, 4), lax.rem(q, 4)

    pairs = [
        (lr_in, lr), (mass_in, mass), (bins_in, bins), (w_in, w), (b_in, b), (ext_in, ext), (ssa_in, ssa),
        (asy_in, asy), (gas_in, gas), (band_in, band), (tau_in, tau), (mask_in, mask), (absb_in, absb),
        (alb_in, alb), (cosz_in, cosz), (sol_in, sol),
    ]
    loads = [pltpu.make_async_copy(src, dst, in_sems.at[i]) for i, (src, dst) in enumerate(pairs)]
    barrier = pltpu.get_barrier_semaphore()

    for i in range(1, 32):
        _, px, py = plane(i)
        pl.semaphore_signal(barrier, inc=1, device_id={"x": px, "y": py}, device_id_type=MESH)
    for i in range(1, 8):
        qh, ql = ring(i)
        pl.semaphore_signal(barrier, inc=1, device_id={"zh": qh, "zl": ql}, device_id_type=MESH)
    pl.semaphore_signal(barrier, inc=1, device_id={"cc": other}, device_id_type=MESH)
    for a in range(4):

        @pl.when(jnp.logical_not(own_piece & (zl == a)))
        def _():
            at = {"zh": lax.rem(x, 2), "cc": lax.div(x, 2), "x": zl, "zl": a}
            pl.semaphore_signal(barrier, inc=1, device_id=at, device_id_type=MESH)

    for load in loads:
        load.start()
    hw_copy = pltpu.make_async_copy(hw.at[pl.ds(2 * cc, 2)], hv, l_hw)
    hw_copy.start()

    for load in loads[:5]:
        load.wait()
    send_features(mass, bins, lr, fs, slot_col)
    spread = (iota((16, COL_DEV), 1) == y * 16 + iota((16, COL_DEV), 0)).astype(BF)
    bs[...] = nn(b[...], spread)
    sender = lax.div(x, 2) == cc
    xb = lax.rem(x, 2)

    @pl.when(own_piece)
    def _():
        pl.semaphore_wait(barrier, 42)

    @pl.when(jnp.logical_not(own_piece))
    def _():
        pl.semaphore_wait(barrier, 43)

    z_steps = (1, 7, 2 + 4 * cc)

    @pl.when(sender)
    def _():
        for i in z_steps:
            qh, ql = ring(i)
            remote(w.at[:, COL_DEV:], wl.at[zl], s_wl, r_wl, zh=qh, zl=ql).start()
        wl[zl] = w[:, COL_DEV:]

    def go_features(i, c):
        p, px, py = plane(i)
        remote(fs.at[p], fr.at[me], s_f, r_f, x=px, y=py).start()
        return c

    lax.fori_loop(1, 32, go_features, 0)
    fr[me] = fs[me]

    @pl.when(sender)
    def _():
        def go(i, c):
            _, px, py = plane(i)
            remote(w.at[:, 0:COL_DEV], wa.at[xb, zl, y], s_w, r_w, x=px, y=py).start()
            remote(bs, br.at[xb, y], s_b, r_b, x=px, y=py).start()
            return c

        lax.fori_loop(1, 32, go, 0)
        wa[xb, zl, y] = w[:, 0:COL_DEV]
        br[xb, y] = bs[...]

    for load in loads[5:]:
        load.wait()
    bcol = evolve_setup(ext, ssa, asy, gas, sol, band, tab, gcol, m0)
    evolve_layers(mass, bins, tau, mask, absb, tab, gcol, opt, refl, trans)

    @pl.when(sender)
    def _():
        wait_bytes(fr.at[0:3], r_wl)
        for i in range(1, 8):
            remote(wl, wb.at[xb, :, y], s_wy, r_wy, y=lax.rem(y + i, 8)).start()
        wb[xb, :, y] = wl[...]

    wait_bytes(fr.at[0:31], r_f)
    got = fr[...].reshape(512, COL_DEV)
    o = iota((COL_DEV, 512), 0)
    source = ((o >> 1) & 31) * 16 + (o >> 6) * 2 + (o & 1)
    shift = iota((COL_DEV, 512), 1) - source
    for a in range(4):
        pick = jnp.where(shift == 4 * a, 1.0, 0.0).astype(BF)
        fz[a] = nn(pick, got).astype(BF)
    for i in (4, 3, 5, 2, 6, 1, 7):
        qh, ql = ring(i)
        remote(fz.at[ql], fx.at[z], s_fz, r_fz, zh=qh, zl=ql).start()
    fx[z] = fz[zl]

    evolve_up(alb, bcol, refl, trans, below)
    evolve_down(sol, cosz, m0, below, trans, down, flux)

    place = jnp.where(iota((256, COL_DEV), 0) == slot_col[...], 1.0, 0.0).astype(BF)
    ts[...] = nt(place, flux[...].astype(BF)).reshape(32, 8, COL_DEV).astype(BF)

    def go_targets(i, c):
        p, px, py = plane(i)
        remote(ts.at[p], tr.at[me], s_t, r_t, x=px, y=py).start()
        return c

    lax.fori_loop(1, 32, go_targets, 0)
    tr[me] = ts[me]

    @pl.when(sender)
    def _():
        wait_bytes(fr.at[0:15], r_w)
        wait_bytes(bpr.at[0:15], r_b)

    @pl.when(jnp.logical_not(sender))
    def _():
        wait_bytes(fr.at[0:16], r_w)
        wait_bytes(bpr.at[0:16], r_b)

    for a in range(2):
        bz[a, zl] = jnp.sum(br[a], axis=0)
    for i in z_steps:
        qh, ql = ring(i)
        remote(wa.at[:, zl], wa.at[:, zl], s_wz, r_wz, zh=qh, zl=ql).start()
        remote(bz.at[:, zl], bz.at[:, zl], s_bz, r_bz, zh=qh, zl=ql).start()

    @pl.when(sender)
    def _():
        wait_bytes(fr.at[0:28], r_wy)
        for i in (1, 3, 2):
            remote(wb.at[xb], wb.at[xb], s_wx, r_wx, x=lax.rem(x + i, 4)).start()

    hw_copy.wait()
    eye = jnp.where(iota((COL_DEV, COL_DEV), 0) == iota((COL_DEV, COL_DEV), 1), 1.0, 0.0).astype(BF)
    for a in range(2):
        hwt[a] = nt(eye, hv[a]).astype(BF)
    wait_bytes(tr.at[0:31], r_t)
    gott = tr[...].astype(F32).reshape(256, COL_DEV).astype(BF)
    ot = iota((64, 256), 0)
    shift_t = iota((64, 256), 1) - ((ot >> 1) * 8 + (ot & 1))
    for a in range(4):
        tz[a] = nn(jnp.where(shift_t == 2 * a, 1.0, 0.0).astype(BF), gott).astype(BF)
    for i in (4, 3, 5, 2, 6, 1, 7):
        qh, ql = ring(i)
        remote(tz.at[ql], tx.at[z], s_tz, r_tz, zh=qh, zl=ql).start()
    tx[z] = tz[zl]

    wait_bytes(fx.at[0:7], r_fz)
    fd = remote(fx, fo, s_fd, r_fd, cc=other)
    fd.start()
    wait_bytes(bz.at[:, 0:3], r_bz)
    for a in range(2):
        for q in range(4):
            biasc[a, q * COL_DEV : (q + 1) * COL_DEV, :] = jnp.broadcast_to(row_to_col(bz[a, q]), (COL_DEV, COL_DEV))
    wait_bytes(wa.at[:, 0:3], r_wz)

    @pl.when(sender)
    def _():
        wait_bytes(wb.at[0], r_wx)

    @pl.when(jnp.logical_not(sender))
    def _():
        wait_bytes(wb, r_wx)

    def gather_x(side, ref):
        for q in range(8):
            for h in range(2):
                xs[side * 2 + q // 4, (q % 4) * 64 : (q % 4 + 1) * 64, h * COL_DEV : (h + 1) * COL_DEV] = ref[
                    q, h * 64 : (h + 1) * 64, :
                ]

    gather_x(0, fx)

    def forward(sb, half, with_slope):
        rows = jnp.concatenate([wa[half].reshape(512, COL_DEV), wb[half].reshape(512, COL_DEV)], axis=1)
        pre[...] = nt(rows, xs[sb])
        for r in range(0, 512, 32):
            v = pre[r : r + 32, :]
            bc = biasc[half, r : r + 32, :]
            v = v + jnp.concatenate([bc, bc], axis=1)
            sq = v * v
            t = jnp.tanh(v * (ROOT + (ROOT * CUBE) * sq))
            cdf = 0.5 + 0.5 * t
            ht[sb, half, r : r + 32, :] = (v * cdf).astype(BF)
            if with_slope:
                slope[sb, r : r + 32, :] = cdf + (0.5 * v) * ((1.0 - t * t) * (ROOT + (3.0 * CUBE * ROOT) * sq))
        return nn(hwt[half], ht[sb, half])

    def forward_block(sb, c):
        pp[sb] = forward(sb, zh, True) + forward(sb, 1 - zh, False)
        return c

    lax.fori_loop(0, 2, forward_block, 0)
    pd = remote(pp.at[0:2], po.at[0:2], s_p, r_p, cc=other)
    pd.start()
    fd.wait()
    gather_x(1, fo)
    lax.fori_loop(2, 4, forward_block, 0)
    pd1 = remote(pp.at[2:4], po.at[2:4], s_p1, r_p1, cc=other)
    pd1.start()

    wait_bytes(tx.at[0:7], r_tz)
    td = remote(tx, to, s_td, r_td, cc=other)
    td.start()
    pd.wait()
    pd1.wait()
    td.wait()
    lane0 = jnp.where(iota((8, COL_DEV), 1) == 0, 1.0, 0.0).astype(BF)
    for sb in range(4):
        src = (tx, tx, to, to)[sb]
        goal = nt(eye, src[(sb % 2) * 4 : (sb % 2) * 4 + 4].reshape(256, COL_DEV))
        flag = nt(lane0, xs[sb, :, COL_DEV:])[0:1, :]
        factor = jnp.where(flag < 1.5, 1.0 / COL_DEV, 0.0)
        gt[sb] = (((pp[sb] + po[(sb + 2) % 4]) - goal) * factor).astype(BF)

    ones = jnp.ones((8, 256), BF)
    for part_of in range(2):
        units = slice(part_of * 256, part_of * 256 + 256)
        brow = jnp.zeros((8, 256), F32)
        for sb in range(4):
            hgrad = nn(hv[zh, units, :], gt[sb])
            pgrad = (hgrad * slope[sb, units, :]).astype(BF)
            term = nn(pgrad, xs[sb])
            ta[...] = term if sb == 0 else ta[...] + term
            brow = brow + nt(ones, pgrad)
        tps[part_of * 16 : part_of * 16 + 16] = ta[...].reshape(16, 16, 256).astype(BF)
        for a in range(2):
            bps[part_of * 2 + a] = brow[0:1, a * COL_DEV : (a + 1) * COL_DEV]

        def go_trunk(i, c, part_of=part_of):
            p = part_of * 16 + lax.rem(me + i, 16)
            px, py = lax.div(p, 8), lax.rem(p, 8)

            @pl.when(p != me)
            def _():
                remote(tps.at[p], tpr.at[me], s_k, r_k, x=px, y=py).start()
                remote(bps.at[px], bpr.at[me], s_kb, r_kb, x=px, y=py).start()

            return c

        lax.fori_loop(0, 16, go_trunk, 0)
    tpr[me] = tps[me]
    bpr[me] = bps[x]

    for half in range(2):
        total = nt(ht[0, half], gt[0])
        for sb in range(1, 4):
            total = total + nt(ht[sb, half], gt[sb])
        hg[half] = total
    hd = remote(hg, head.at[pl.ds(2 * cc, 2)], s_h, r_h, cc=other)
    hd.start()
    hl = pltpu.make_async_copy(hg, head.at[pl.ds(2 * cc, 2)], l_h)
    hl.start()

    wait_bytes(tpr.at[0:31], r_k)
    wait_bytes(bpr.at[0:31], r_kb)
    fsum[...] = jnp.sum(tpr[...].astype(F32), axis=0)
    fbsum[...] = jnp.sum(bpr[...], axis=0)
    for qh in range(2):
        for qc in range(2):
            mine = own_piece & (zh == qh) & (cc == qc)

            @pl.when(jnp.logical_not(mine))
            def _():
                at = dict(zh=qh, cc=qc, x=part, zl=x)
                remote(fsum, gr.at[zl], s_e, r_e, **at).start()
                remote(fbsum, gb.at[zl], s_eb, r_eb, **at).start()

            @pl.when(mine)
            def _():
                gr[zl] = fsum[...]
                gb[zl] = fbsum[...]

    @pl.when(own_piece)
    def _():
        wait_bytes(gr.at[0:3], r_e)
        wait_bytes(gb.at[0:3], r_eb)

    @pl.when(jnp.logical_not(own_piece))
    def _():
        wait_bytes(gr, r_e)
        wait_bytes(gb, r_eb)

    tg[...] = (gr[0] + gr[1]) + (gr[2] + gr[3])
    brows = (gb[0] + gb[1]) + (gb[2] + gb[3])
    kept = jnp.where(lax.div(iota((1, COL_DEV), 1), 16) == y, brows, 0.0)
    bias = kept[:, 0:16]
    for a in range(1, 8):
        bias = bias + kept[:, a * 16 : (a + 1) * 16]
    bg[...] = bias

    hl.wait()
    hd.wait_send()
    wait_bytes(head.at[pl.ds(2 * other, 2)], r_h)

    @pl.when(sender)
    def _():
        wait_bytes(fr.at[0:31], s_w)
        wait_bytes(bpr.at[0:31], s_b)
        wait_bytes(fr.at[0:3], s_wl)
        wait_bytes(fr.at[0:28], s_wy)
        wait_bytes(xs.at[0:3], s_wx)

    wait_bytes(fs.at[0:31], s_f)
    wait_bytes(wa.at[:, 0:3], s_wz)
    wait_bytes(bz.at[:, 0:3], s_bz)
    wait_bytes(fx.at[0:7], s_fz)
    wait_bytes(ts.at[0:31], s_t)
    wait_bytes(tx.at[0:7], s_tz)
    wait_bytes(tps.at[0:31], s_k)
    wait_bytes(bpr.at[0:31], s_kb)

    @pl.when(own_piece)
    def _():
        wait_bytes(gr.at[0:3], s_e)
        wait_bytes(gb.at[0:3], s_eb)

    @pl.when(jnp.logical_not(own_piece))
    def _():
        wait_bytes(gr, s_e)
        wait_bytes(gb, s_eb)


def copy_out(flux_in, head_in, tg_in, bg_in, flux, head, tg, bg, vflux, vhead, vtg, vbg, sems):
    trips = [(head_in.at[i], vhead.at[i], head.at[i]) for i in range(4)]
    trips += [(flux_in, vflux, flux), (tg_in, vtg, tg), (bg_in, vbg, bg)]
    ins = [pltpu.make_async_copy(a, b, sems.at[0, i]) for i, (a, b, _) in enumerate(trips)]
    outs = [pltpu.make_async_copy(b, c, sems.at[1, i]) for i, (_, b, c) in enumerate(trips)]
    for copy in ins:
        copy.start()
    for copy, out in zip(ins, outs):
        copy.wait()
        out.start()
    for out in outs:
        out.wait()


def per_device(mass, bins, tau, mask, absb, alb, cosz, ext, ssa, asy, gas, sol, band, lr, w, b, hw):
    vm = pl.BlockSpec(memory_space=pltpu.VMEM)
    hbm = pl.BlockSpec(memory_space=pl.ANY)
    v = pltpu.VMEM
    c = COL_DEV
    flux, head, tg, bg = pl.pallas_call(
        kernel,
        out_shape=(
            jax.ShapeDtypeStruct((4 * LEV, c), F32),
            jax.ShapeDtypeStruct((4, 512, c), F32),
            jax.ShapeDtypeStruct((16, 256), F32),
            jax.ShapeDtypeStruct((1, 16), F32),
        ),
        in_specs=[hbm] * 17,
        out_specs=(vm, hbm, vm, vm),
        scratch_shapes=[
            v((MODES, LEV, c), F32), v((MODES, LEV, c), jnp.int32), v((LEV, c), F32), v((1, c), jnp.int32),
            v((LEV, c), F32), v((NB, c), F32), v((1, c), F32), v((G, 256), F32), v((G, 256), F32), v((G, 256), F32),
            v((1, G), F32), v((1, G), F32), v((1, G), jnp.int32), v((1, c), jnp.int32), v((16, 256), BF), v((1, 16), BF),
            pltpu.SemaphoreType.DMA((16,)),
            v((3 * G, MODES * BINS), BF), v((G, c), F32), v((G, c), F32), v((3 * G, LU * c), F32),
            v((LEV, G, c), F32), v((LEV, G, c), F32), v((LEV + 1, G, c), F32), v((G, c), F32),
            v((1, c), jnp.int32),
            v((32, 16, c), BF), v((32, 16, c), BF), v((4, 128, c), BF), v((8, 128, c), BF), v((8, 128, c), BF),
            v((32, 8, c), BF), v((32, 8, c), BF), v((4, 64, c), BF), v((8, 64, c), BF), v((8, 64, c), BF),
            v((2, 4, 8, 16, c), BF), v((2, 4, 8, 16, c), BF), v((4, 16, c), BF), v((1, c), F32), v((2, 8, 1, c), F32), v((2, 4, 1, c), F32),
            v((2, 512, c), BF), v((2, c, 512), BF), v((2, 512, c), F32),
            v((4, 256, 256), BF), v((512, 256), F32), v((4, 512, 256), F32), v((4, 2, 512, 256), BF),
            v((4, c, 256), F32), v((4, c, 256), F32), v((4, c, 256), BF), v((256, 256), F32),
            v((32, 16, 256), BF), v((4, 1, c), F32), v((32, 16, 256), BF), v((32, 1, c), F32),
            v((16, 256), F32), v((1, c), F32), v((4, 16, 256), F32), v((4, 1, c), F32), v((2, 512, c), F32),
        ] + [pltpu.SemaphoreType.DMA] * 42,
        compiler_params=pltpu.CompilerParams(collective_id=0, has_side_effects=True),
    )(
        mass, bins, tau, mask[None], absb, alb, cosz[None], ext, ssa, asy, gas[None], sol[None], band[None],
        lr.reshape(1, c), w, b[None], hw.reshape(4, 512, c),
    )
    flux, head, tg, bg = pl.pallas_call(
        copy_out,
        out_shape=tuple(jax.ShapeDtypeStruct(a.shape, F32) for a in (flux, head, tg, bg)),
        in_specs=[hbm] * 4,
        out_specs=(hbm,) * 4,
        scratch_shapes=[v(a.shape, F32) for a in (flux, head, tg, bg)] + [pltpu.SemaphoreType.DMA((2, 7))],
    )(flux, head, tg, bg)
    return flux, head.reshape(1, 2048, c), tg, bg[0]


def solution(mesh):
    split = Mesh(mesh.devices.reshape(2, 2, 4, 4, 8), GRP_LRN)
    placed = (
        P(None, None, GRP_LRN),
        P(None, None, GRP_LRN),
        P(None, GRP_LRN),
        P(GRP_LRN),
        P(None, GRP_LRN),
        P(None, GRP_LRN),
        P(GRP_LRN),
        P(),
        P(),
        P(),
        P(),
        P(),
        P(),
        P(GRP_LRN, None),
        P(LRN, None),
        P(LRN),
        P(LRN, None, None),
    )
    return jax.shard_map(
        per_device,
        mesh=split,
        in_specs=placed,
        out_specs=(P(None, GRP_LRN), P(LRN, None, None), P(LRN, None), P(LRN)),
        check_vma=False,
    )
```

```python
import math

import jax
import jax.numpy as jnp
from jax import lax
from jax.experimental import pallas as pl
from jax.experimental.pallas import tpu as pltpu
from jax.sharding import Mesh
from jax.sharding import PartitionSpec as P

MODES = 4
BINS = 64
G = 112
NB = 14
LEV = 32
COL_DEV = 128
LRN = ("x", "zl", "y")
GRP_LRN = ("zh", "cc", "x", "zl", "y")
MESH = pl.DeviceIdType.MESH
BF = jnp.bfloat16
F32 = jnp.float32
CLOUD_SSA = 0.99
CLOUD_ASYM = 0.85


def nt(a, b):
    return lax.dot_general(a, b, (((1,), (1,)), ((), ())), preferred_element_type=F32)


def nn(a, b):
    return jnp.dot(a, b, preferred_element_type=F32)


def iota(shape, dim):
    return lax.broadcasted_iota(jnp.int32, shape, dim)


def row_to_col(row):
    n = row.shape[1]
    rows = lax.broadcasted_iota(jnp.int32, (n, n), 0)
    cols = lax.broadcasted_iota(jnp.int32, (n, n), 1)
    return jnp.sum(jnp.where(rows == cols, jnp.broadcast_to(row, (n, n)), 0.0), axis=1, keepdims=True)


def evolve_setup(ext, ssa, asy, gas, sol, band, tab, gcol, m0):
    e = ext[...]
    s = e * ssa[...]
    tab[0:G, :] = e.astype(jnp.bfloat16)
    tab[G : 2 * G, :] = s.astype(jnp.bfloat16)
    tab[2 * G : 3 * G, :] = (s * asy[...]).astype(jnp.bfloat16)
    gcol[...] = jnp.broadcast_to(row_to_col(gas[...]), (G, COL_DEV))
    bcol = row_to_col(band[...].astype(jnp.float32))
    m0[...] = jnp.broadcast_to(jnp.where(bcol < NB // 2, 1.0, 0.0), (G, COL_DEV))
    return bcol


CH = 8
LU = 4


def evolve_layers(mass, bins, tau, mask, absb, tab, gcol, opt, refl, trans):
    labels = lax.broadcasted_iota(jnp.int32, (BINS, COL_DEV), 0)
    cloudy_on = mask[...].astype(jnp.float32)

    def body(step, carry):
        pieces = []
        for u in range(LU):
            l = step * LU + u
            modes = []
            for m in range(MODES):
                load = mass[m, pl.ds(l, 1), :]
                hot = bins[m, pl.ds(l, 1), :] == labels
                modes.append(jnp.where(hot, jnp.broadcast_to(load, (BINS, COL_DEV)), 0.0))
            pieces.append(jnp.concatenate(modes, axis=0).astype(jnp.bfloat16))
        weights = jnp.concatenate(pieces, axis=1)
        opt[...] = jnp.dot(tab[...], weights, preferred_element_type=jnp.float32)
        for u in range(LU):
            l = step * LU + u
            cl = tau[pl.ds(l, 1), :] * cloudy_on
            ab = absb[pl.ds(l, 1), :]
            c1 = CLOUD_SSA * cl
            c2 = CLOUD_SSA * CLOUD_ASYM * cl
            lanes = slice(u * COL_DEV, (u + 1) * COL_DEV)
            for g in range(0, G, CH):
                d = opt[g : g + CH, lanes] + cl + gcol[g : g + CH, :] * ab
                s = opt[G + g : G + g + CH, lanes] + c1
                f = opt[2 * G + g : 2 * G + g + CH, lanes] + c2
                ds, df = d - s, d - f
                k = 2.0 * jnp.sqrt(ds * df)
                g1 = ds + df
                e = jnp.exp(-k)
                sq = e * e
                r = 1.0 / ((k + g1) + (k - g1) * sq)
                refl[l, g : g + CH, :] = (s - f) * (1.0 - sq) * r
                trans[l, g : g + CH, :] = 2.0 * k * e * r
        return carry

    lax.fori_loop(0, LEV // LU, body, 0)


def evolve_up(alb, bcol, refl, trans, below):
    surface = jnp.zeros((G, COL_DEV), jnp.float32)
    for b in range(NB):
        surface = jnp.where(bcol == float(b), jnp.broadcast_to(alb[b : b + 1, :], (G, COL_DEV)), surface)
    below[LEV] = surface

    def body(step, carry):
        l = LEV - 1 - step
        layer = [(refl[l, g : g + CH, :], trans[l, g : g + CH, :]) for g in range(0, G, CH)]
        nxt, ratio = [], []
        for b, (r, t) in zip(carry, layer):
            q = t / (1.0 - r * b)
            ratio.append(q)
            nxt.append(r + t * b * q)
        for i, g in enumerate(range(0, G, CH)):
            below[l, g : g + CH, :] = nxt[i]
            trans[l, g : g + CH, :] = ratio[i]
        return tuple(nxt)

    lax.fori_loop(0, LEV, body, tuple(surface[g : g + CH, :] for g in range(0, G, CH)))


def evolve_down(sol, cosz, m0, below, trans, down, flux):
    cosv = cosz[...]
    scol = row_to_col(sol[...])
    down[...] = jnp.broadcast_to(scol, (G, COL_DEV)) * cosv
    scale = 2.0 / G

    def body(l, carry):
        acc = [jnp.zeros((CH, COL_DEV), jnp.float32) for _ in range(4)]
        for g in range(0, G, CH):
            rows = slice(g, g + CH)
            now = down[rows, :]
            low = m0[rows, :]
            up = below[l, rows, :] * now
            nxt = trans[l, rows, :] * now
            down[rows, :] = nxt
            nl, ul = nxt * low, up * low
            acc[0] = acc[0] + nl
            acc[1] = acc[1] + ul
            acc[2] = acc[2] + (nxt - nl)
            acc[3] = acc[3] + (up - ul)
        for i in range(4):
            flux[pl.ds(i * LEV + l, 1), :] = jnp.sum(acc[i], axis=0, keepdims=True) * scale
        return carry

    lax.fori_loop(0, LEV, body, 0)


EMPTY = 2.0
ROOT = math.sqrt(2.0 / math.pi)
CUBE = 0.044715


def remote(src, dst, send, recv, **at):
    return pltpu.make_async_remote_copy(
        src_ref=src, dst_ref=dst, send_sem=send, recv_sem=recv, device_id=at, device_id_type=MESH
    )


STEPS = sorted(
    ((dx, dy) for dx in range(4) for dy in range(8) if dx or dy),
    key=lambda s: (-min(s[0], 4 - s[0]) - min(s[1], 8 - s[1]), min(s[1], 8 - s[1]), s[0], s[1]),
)


def wait_bytes(ref, sem):
    pltpu.make_async_copy(ref, ref, sem).wait()


def send_features(mass, bins, lr, fs, slot_col):
    row = lr[...]
    col = row_to_col(row.astype(F32))
    same = jnp.broadcast_to(col, (COL_DEV, COL_DEV)) == jnp.broadcast_to(row.astype(F32), (COL_DEV, COL_DEV))
    before = iota((COL_DEV, COL_DEV), 0) < iota((COL_DEV, COL_DEV), 1)
    rank = jnp.sum(jnp.where(same & before, 1.0, 0.0), axis=0, keepdims=True).astype(jnp.int32)
    peer = (row >> 5) * 8 + (row & 7)
    key = peer * 16 + ((row >> 3) & 3) * 4 + rank
    slot_col[...] = peer * 8 + ((row >> 3) & 3) * 2 + rank
    first = ((jnp.log(mass[...]) + 4.6) / 1.4).reshape(MODES * LEV, COL_DEV).astype(BF)
    half = BINS / 2
    second = ((bins[...].astype(F32) - half) / half).reshape(MODES * LEV, COL_DEV).astype(BF)
    rows = iota((512, COL_DEV), 0)
    hot0 = jnp.where(rows == key, 1.0, 0.0).astype(BF)
    hot1 = jnp.where(rows == key + 2, 1.0, 0.0).astype(BF)
    data = nt(hot0, first) + nt(hot1, second)
    filled = nn(hot0 + hot1, jnp.ones((COL_DEV, COL_DEV), BF))
    empty = (filled < 0.5) & (iota((512, COL_DEV), 1) == 0)
    fs[...] = jnp.where(empty, EMPTY, data).reshape(32, 16, COL_DEV).astype(BF)


def kernel(
    mass_in, bins_in, tau_in, mask_in, absb_in, alb_in, cosz_in, ext_in, ssa_in, asy_in, gas_in, sol_in, band_in,
    lr_in, w_in, b_in, hw,
    flux, head, tg, bg,
    mass, bins, tau, mask, absb, alb, cosz, ext, ssa, asy, gas, sol, band, lr, w, b, in_sems,
    tab, gcol, m0, opt, refl, trans, below, down,
    slot_col, fs, fr, fz, fx, fo, ts, tr, tz, tx, to, wa, wb, wl, bs, br, bz, hv, hwt, biasc,
    xs, pre, slope, ht, pp, po, gt, ta, tps, bps, tpr, bpr, fsum, fbsum, gr, gb, hg,
    s_w, r_w, s_b, r_b, s_f, r_f, s_wz, r_wz, s_bz, r_bz, s_wl, r_wl, s_wy, r_wy, s_wx, r_wx, s_fz, r_fz, s_fd, r_fd,
    s_t, r_t, s_tz, r_tz, s_td, r_td, s_h, r_h, l_h, l_hw,
    s_k, r_k, s_kb, r_kb, s_e, r_e, s_eb, r_eb, s_p, r_p,
):
    zh, cc, x, zl, y = (lax.axis_index(a) for a in GRP_LRN)
    other = 1 - cc
    me = x * 8 + y
    z = zh * 4 + zl
    part = 2 * cc + zh
    own_piece = (part == x) & (x == zl)

    def plane(step):
        px, py = lax.rem(x + step[0], 4), lax.rem(y + step[1], 8)
        return px * 8 + py, px, py

    def ring(i):
        q = lax.rem(z + i, 8)
        return lax.div(q, 4), lax.rem(q, 4)

    pairs = [
        (lr_in, lr), (mass_in, mass), (bins_in, bins), (w_in, w), (b_in, b), (ext_in, ext), (ssa_in, ssa),
        (asy_in, asy), (gas_in, gas), (band_in, band), (tau_in, tau), (mask_in, mask), (absb_in, absb),
        (alb_in, alb), (cosz_in, cosz), (sol_in, sol),
    ]
    loads = [pltpu.make_async_copy(src, dst, in_sems.at[i]) for i, (src, dst) in enumerate(pairs)]
    barrier = pltpu.get_barrier_semaphore()

    for step in STEPS:
        _, px, py = plane(step)
        pl.semaphore_signal(barrier, inc=1, device_id={"x": px, "y": py}, device_id_type=MESH)
    for i in range(1, 8):
        qh, ql = ring(i)
        pl.semaphore_signal(barrier, inc=1, device_id={"zh": qh, "zl": ql}, device_id_type=MESH)
    pl.semaphore_signal(barrier, inc=1, device_id={"cc": other}, device_id_type=MESH)
    for a in range(4):

        @pl.when(jnp.logical_not(own_piece & (zl == a)))
        def _():
            at = {"zh": lax.rem(x, 2), "cc": lax.div(x, 2), "x": zl, "zl": a}
            pl.semaphore_signal(barrier, inc=1, device_id=at, device_id_type=MESH)

    for load in loads:
        load.start()
    hw_copy = pltpu.make_async_copy(hw.at[pl.ds(2 * cc, 2)], hv, l_hw)
    hw_copy.start()

    for load in loads[:5]:
        load.wait()
    send_features(mass, bins, lr, fs, slot_col)
    spread = (iota((16, COL_DEV), 1) == y * 16 + iota((16, COL_DEV), 0)).astype(BF)
    bs[...] = nn(b[...], spread)
    sender = lax.div(x, 2) == cc
    xb = lax.rem(x, 2)

    @pl.when(own_piece)
    def _():
        pl.semaphore_wait(barrier, 42)

    @pl.when(jnp.logical_not(own_piece))
    def _():
        pl.semaphore_wait(barrier, 43)

    z_steps = (1, 7, 2 + 4 * cc)

    @pl.when(sender)
    def _():
        for i in z_steps:
            qh, ql = ring(i)
            remote(w.at[:, COL_DEV:], wl.at[zl], s_wl, r_wl, zh=qh, zl=ql).start()
        wl[zl] = w[:, COL_DEV:]

    for step in STEPS:
        p, px, py = plane(step)
        remote(fs.at[p], fr.at[me], s_f, r_f, x=px, y=py).start()
    fr[me] = fs[me]

    @pl.when(sender)
    def _():
        for step in STEPS:
            _, px, py = plane(step)
            remote(w.at[:, 0:COL_DEV], wa.at[xb, zl, y], s_w, r_w, x=px, y=py).start()
            remote(bs, br.at[xb, y], s_b, r_b, x=px, y=py).start()
        wa[xb, zl, y] = w[:, 0:COL_DEV]
        br[xb, y] = bs[...]

    for load in loads[5:]:
        load.wait()
    bcol = evolve_setup(ext, ssa, asy, gas, sol, band, tab, gcol, m0)
    evolve_layers(mass, bins, tau, mask, absb, tab, gcol, opt, refl, trans)

    @pl.when(sender)
    def _():
        wait_bytes(fr.at[0:3], r_wl)
        for i in range(1, 8):
            remote(wl, wb.at[xb, :, y], s_wy, r_wy, y=lax.rem(y + i, 8)).start()
        wb[xb, :, y] = wl[...]

    wait_bytes(fr.at[0:31], r_f)
    got = fr[...].reshape(512, COL_DEV)
    o = iota((COL_DEV, 512), 0)
    source = ((o >> 1) & 31) * 16 + (o >> 6) * 2 + (o & 1)
    shift = iota((COL_DEV, 512), 1) - source
    for a in range(4):
        pick = jnp.where(shift == 4 * a, 1.0, 0.0).astype(BF)
        fz[a] = nn(pick, got).astype(BF)
    for i in (4, 3, 5, 2, 6, 1, 7):
        qh, ql = ring(i)
        remote(fz.at[ql], fx.at[z], s_fz, r_fz, zh=qh, zl=ql).start()
    fx[z] = fz[zl]

    evolve_up(alb, bcol, refl, trans, below)
    evolve_down(sol, cosz, m0, below, trans, down, flux)

    place = jnp.where(iota((256, COL_DEV), 0) == slot_col[...], 1.0, 0.0).astype(BF)
    ts[...] = nt(place, flux[...].astype(BF)).reshape(32, 8, COL_DEV).astype(BF)

    for step in STEPS:
        p, px, py = plane(step)
        remote(ts.at[p], tr.at[me], s_t, r_t, x=px, y=py).start()
    tr[me] = ts[me]

    @pl.when(sender)
    def _():
        wait_bytes(fr.at[0:15], r_w)
        wait_bytes(bpr.at[0:15], r_b)

    @pl.when(jnp.logical_not(sender))
    def _():
        wait_bytes(fr.at[0:16], r_w)
        wait_bytes(bpr.at[0:16], r_b)

    for a in range(2):
        bz[a, zl] = jnp.sum(br[a], axis=0)
    for i in z_steps:
        qh, ql = ring(i)
        remote(wa.at[:, zl], wa.at[:, zl], s_wz, r_wz, zh=qh, zl=ql).start()
        remote(bz.at[:, zl], bz.at[:, zl], s_bz, r_bz, zh=qh, zl=ql).start()

    @pl.when(sender)
    def _():
        wait_bytes(fr.at[0:28], r_wy)
        for i in (1, 3, 2):
            remote(wb.at[xb], wb.at[xb], s_wx, r_wx, x=lax.rem(x + i, 4)).start()

    hw_copy.wait()
    eye = jnp.where(iota((COL_DEV, COL_DEV), 0) == iota((COL_DEV, COL_DEV), 1), 1.0, 0.0).astype(BF)
    for a in range(2):
        hwt[a] = (0.5 * nt(eye, hv[a])).astype(BF)
    wait_bytes(tr.at[0:31], r_t)
    gott = tr[...].astype(F32).reshape(256, COL_DEV).astype(BF)
    ot = iota((64, 256), 0)
    shift_t = iota((64, 256), 1) - ((ot >> 1) * 8 + (ot & 1))
    for a in range(4):
        tz[a] = nn(jnp.where(shift_t == 2 * a, 1.0, 0.0).astype(BF), gott).astype(BF)
    for i in (4, 3, 5, 2, 6, 1, 7):
        qh, ql = ring(i)
        remote(tz.at[ql], tx.at[z], s_tz, r_tz, zh=qh, zl=ql).start()
    tx[z] = tz[zl]

    wait_bytes(fx.at[0:7], r_fz)
    fd = remote(fx, fo, s_fd, r_fd, cc=other)
    fd.start()
    wait_bytes(bz.at[:, 0:3], r_bz)
    for a in range(2):
        for q in range(4):
            biasc[a, q * COL_DEV : (q + 1) * COL_DEV, :] = jnp.broadcast_to(row_to_col(bz[a, q]), (COL_DEV, COL_DEV))
    wait_bytes(wa.at[:, 0:3], r_wz)

    @pl.when(sender)
    def _():
        wait_bytes(wb.at[0], r_wx)

    @pl.when(jnp.logical_not(sender))
    def _():
        wait_bytes(wb, r_wx)

    def gather_x(side, ref):
        for q in range(8):
            for h in range(2):
                xs[side * 2 + q // 4, (q % 4) * 64 : (q % 4 + 1) * 64, h * COL_DEV : (h + 1) * COL_DEV] = ref[
                    q, h * 64 : (h + 1) * 64, :
                ]

    gather_x(0, fx)

    def forward(sb, half, with_slope):
        rows = jnp.concatenate([wa[half].reshape(512, COL_DEV), wb[half].reshape(512, COL_DEV)], axis=1)
        pre[...] = nt(rows, xs[sb])
        for r in range(0, 512, 32):
            v = pre[r : r + 32, :]
            bc = biasc[half, r : r + 32, :]
            v = v + jnp.concatenate([bc, bc], axis=1)
            sq = v * v
            t = jnp.tanh(v * (ROOT + (ROOT * CUBE) * sq))
            up = 1.0 + t
            ht[sb, half, r : r + 32, :] = (v * up).astype(BF)
            if with_slope:
                slope[sb, r : r + 32, :] = up + v * ((1.0 - t * t) * (ROOT + (3.0 * CUBE * ROOT) * sq))
        return nn(hwt[half], ht[sb, half])

    def swap(sb):
        return remote(pp.at[sb], po.at[sb], s_p.at[sb], r_p.at[sb], cc=other)

    def forward_block(sb, c):
        pp[sb] = forward(sb, zh, True) + forward(sb, 1 - zh, False)
        swap(sb).start()
        return c

    lax.fori_loop(0, 2, forward_block, 0)
    fd.wait()
    gather_x(1, fo)
    lax.fori_loop(2, 3, forward_block, 0)
    wait_bytes(tx.at[0:7], r_tz)
    td = remote(tx, to, s_td, r_td, cc=other)
    td.start()
    lax.fori_loop(3, 4, forward_block, 0)
    lane0 = jnp.where(iota((8, COL_DEV), 1) == 0, 1.0, 0.0).astype(BF)

    def pred_grad(sb):
        src = (tx, tx, to, to)[sb]
        goal = nt(eye, src[(sb % 2) * 4 : (sb % 2) * 4 + 4].reshape(256, COL_DEV))
        flag = nt(lane0, xs[sb, :, COL_DEV:])[0:1, :]
        factor = jnp.where(flag < 1.5, 1.0 / COL_DEV, 0.0)
        gt[sb] = (((pp[sb] + po[(sb + 2) % 4]) - goal) * factor).astype(BF)

    ones = jnp.ones((8, 256), BF)

    def backward(sb, units):
        hgrad = nn(hv[zh, units, :], gt[sb])
        pgrad = ((0.5 * hgrad) * slope[sb, units, :]).astype(BF)
        return nn(pgrad, xs[sb]), nt(ones, pgrad)

    td.wait()
    for sb in (2, 3):
        swap(sb - 2).wait_recv()
        pred_grad(sb)
    brows = []
    for part_of in range(2):
        units = slice(part_of * 256, part_of * 256 + 256)
        term, brow = backward(2, units)
        ta[units, :] = term
        term, more = backward(3, units)
        ta[units, :] = ta[units, :] + term
        brows.append(brow + more)
    for sb in (0, 1):
        swap(sb + 2).wait_recv()
        pred_grad(sb)
    for part_of in range(2):
        units = slice(part_of * 256, part_of * 256 + 256)
        brow = brows[part_of]
        for sb in (0, 1):
            term, more = backward(sb, units)
            ta[units, :] = ta[units, :] + term
            brow = brow + more
        tps[part_of * 16 : part_of * 16 + 16] = ta[units, :].reshape(16, 16, 256).astype(BF)
        for a in range(2):
            bps[part_of * 2 + a] = brow[0:1, a * COL_DEV : (a + 1) * COL_DEV]

        for dy in (4, 3, 5, 2, 6, 1, 7, 0):
            for px in (part_of * 2, part_of * 2 + 1):
                py = lax.rem(y + dy, 8)
                p = px * 8 + py

                def send(p=p, px=px, py=py):
                    remote(tps.at[p], tpr.at[me], s_k, r_k, x=px, y=py).start()
                    remote(bps.at[px], bpr.at[me], s_kb, r_kb, x=px, y=py).start()

                if dy:
                    send()
                else:
                    pl.when(x != px)(send)
    tpr[me] = tps[me]
    bpr[me] = bps[x]

    for half in range(2):
        total = nt(ht[0, half], gt[0])
        for sb in range(1, 4):
            total = total + nt(ht[sb, half], gt[sb])
        hg[half] = 0.5 * total
    hd = remote(hg, head.at[pl.ds(2 * cc, 2)], s_h, r_h, cc=other)
    hd.start()
    hl = pltpu.make_async_copy(hg, head.at[pl.ds(2 * cc, 2)], l_h)
    hl.start()

    wait_bytes(tpr.at[0:31], r_k)
    wait_bytes(bpr.at[0:31], r_kb)
    fsum[...] = jnp.sum(tpr[...].astype(F32), axis=0)
    fbsum[...] = jnp.sum(bpr[...], axis=0)
    for qh in range(2):
        for qc in range(2):
            mine = own_piece & (zh == qh) & (cc == qc)

            @pl.when(jnp.logical_not(mine))
            def _():
                at = dict(zh=qh, cc=qc, x=part, zl=x)
                remote(fsum, gr.at[zl], s_e, r_e, **at).start()
                remote(fbsum, gb.at[zl], s_eb, r_eb, **at).start()

            @pl.when(mine)
            def _():
                gr[zl] = fsum[...]
                gb[zl] = fbsum[...]

    @pl.when(own_piece)
    def _():
        wait_bytes(gr.at[0:3], r_e)
        wait_bytes(gb.at[0:3], r_eb)

    @pl.when(jnp.logical_not(own_piece))
    def _():
        wait_bytes(gr, r_e)
        wait_bytes(gb, r_eb)

    tg[...] = (gr[0] + gr[1]) + (gr[2] + gr[3])
    brows = (gb[0] + gb[1]) + (gb[2] + gb[3])
    kept = jnp.where(lax.div(iota((1, COL_DEV), 1), 16) == y, brows, 0.0)
    bias = kept[:, 0:16]
    for a in range(1, 8):
        bias = bias + kept[:, a * 16 : (a + 1) * 16]
    bg[...] = bias

    hl.wait()
    hd.wait_send()
    for sb in range(4):
        swap(sb).wait_send()
    wait_bytes(head.at[pl.ds(2 * other, 2)], r_h)

    @pl.when(sender)
    def _():
        wait_bytes(fr.at[0:31], s_w)
        wait_bytes(bpr.at[0:31], s_b)
        wait_bytes(fr.at[0:3], s_wl)
        wait_bytes(fr.at[0:28], s_wy)
        wait_bytes(xs.at[0:3], s_wx)

    wait_bytes(fs.at[0:31], s_f)
    wait_bytes(wa.at[:, 0:3], s_wz)
    wait_bytes(bz.at[:, 0:3], s_bz)
    wait_bytes(fx.at[0:7], s_fz)
    wait_bytes(ts.at[0:31], s_t)
    wait_bytes(tx.at[0:7], s_tz)
    wait_bytes(tps.at[0:31], s_k)
    wait_bytes(bpr.at[0:31], s_kb)

    @pl.when(own_piece)
    def _():
        wait_bytes(gr.at[0:3], s_e)
        wait_bytes(gb.at[0:3], s_eb)

    @pl.when(jnp.logical_not(own_piece))
    def _():
        wait_bytes(gr, s_e)
        wait_bytes(gb, s_eb)


def copy_out(flux_in, head_in, tg_in, bg_in, flux, head, tg, bg, vflux, vhead, vtg, vbg, sems):
    trips = [(head_in.at[i], vhead.at[i], head.at[i]) for i in range(4)]
    trips += [(flux_in, vflux, flux), (tg_in, vtg, tg), (bg_in, vbg, bg)]
    ins = [pltpu.make_async_copy(a, b, sems.at[0, i]) for i, (a, b, _) in enumerate(trips)]
    outs = [pltpu.make_async_copy(b, c, sems.at[1, i]) for i, (_, b, c) in enumerate(trips)]
    for copy in ins:
        copy.start()
    for copy, out in zip(ins, outs):
        copy.wait()
        out.start()
    for out in outs:
        out.wait()


def per_device(mass, bins, tau, mask, absb, alb, cosz, ext, ssa, asy, gas, sol, band, lr, w, b, hw):
    vm = pl.BlockSpec(memory_space=pltpu.VMEM)
    hbm = pl.BlockSpec(memory_space=pl.ANY)
    v = pltpu.VMEM
    c = COL_DEV
    flux, head, tg, bg = pl.pallas_call(
        kernel,
        out_shape=(
            jax.ShapeDtypeStruct((4 * LEV, c), F32),
            jax.ShapeDtypeStruct((4, 512, c), F32),
            jax.ShapeDtypeStruct((16, 256), F32),
            jax.ShapeDtypeStruct((1, 16), F32),
        ),
        in_specs=[hbm] * 17,
        out_specs=(vm, hbm, vm, vm),
        scratch_shapes=[
            v((MODES, LEV, c), F32), v((MODES, LEV, c), jnp.int32), v((LEV, c), F32), v((1, c), jnp.int32),
            v((LEV, c), F32), v((NB, c), F32), v((1, c), F32), v((G, 256), F32), v((G, 256), F32), v((G, 256), F32),
            v((1, G), F32), v((1, G), F32), v((1, G), jnp.int32), v((1, c), jnp.int32), v((16, 256), BF), v((1, 16), BF),
            pltpu.SemaphoreType.DMA((16,)),
            v((3 * G, MODES * BINS), BF), v((G, c), F32), v((G, c), F32), v((3 * G, LU * c), F32),
            v((LEV, G, c), F32), v((LEV, G, c), F32), v((LEV + 1, G, c), F32), v((G, c), F32),
            v((1, c), jnp.int32),
            v((32, 16, c), BF), v((32, 16, c), BF), v((4, 128, c), BF), v((8, 128, c), BF), v((8, 128, c), BF),
            v((32, 8, c), BF), v((32, 8, c), BF), v((4, 64, c), BF), v((8, 64, c), BF), v((8, 64, c), BF),
            v((2, 4, 8, 16, c), BF), v((2, 4, 8, 16, c), BF), v((4, 16, c), BF), v((1, c), F32), v((2, 8, 1, c), F32), v((2, 4, 1, c), F32),
            v((2, 512, c), BF), v((2, c, 512), BF), v((2, 512, c), F32),
            v((4, 256, 256), BF), v((512, 256), F32), v((4, 512, 256), F32), v((4, 2, 512, 256), BF),
            v((4, c, 256), F32), v((4, c, 256), F32), v((4, c, 256), BF), v((512, 256), F32),
            v((32, 16, 256), BF), v((4, 1, c), F32), v((32, 16, 256), BF), v((32, 1, c), F32),
            v((16, 256), F32), v((1, c), F32), v((4, 16, 256), F32), v((4, 1, c), F32), v((2, 512, c), F32),
        ] + [pltpu.SemaphoreType.DMA] * 38 + [pltpu.SemaphoreType.DMA((4,))] * 2,
        compiler_params=pltpu.CompilerParams(collective_id=0, has_side_effects=True),
    )(
        mass, bins, tau, mask[None], absb, alb, cosz[None], ext, ssa, asy, gas[None], sol[None], band[None],
        lr.reshape(1, c), w, b[None], hw.reshape(4, 512, c),
    )
    flux, head, tg, bg = pl.pallas_call(
        copy_out,
        out_shape=tuple(jax.ShapeDtypeStruct(a.shape, F32) for a in (flux, head, tg, bg)),
        in_specs=[hbm] * 4,
        out_specs=(hbm,) * 4,
        scratch_shapes=[v(a.shape, F32) for a in (flux, head, tg, bg)] + [pltpu.SemaphoreType.DMA((2, 7))],
    )(flux, head, tg, bg)
    return flux, head.reshape(1, 2048, c), tg, bg[0]


def solution(mesh):
    split = Mesh(mesh.devices.reshape(2, 2, 4, 4, 8), GRP_LRN)
    placed = (
        P(None, None, GRP_LRN),
        P(None, None, GRP_LRN),
        P(None, GRP_LRN),
        P(GRP_LRN),
        P(None, GRP_LRN),
        P(None, GRP_LRN),
        P(GRP_LRN),
        P(),
        P(),
        P(),
        P(),
        P(),
        P(),
        P(GRP_LRN, None),
        P(LRN, None),
        P(LRN),
        P(LRN, None, None),
    )
    return jax.shard_map(
        per_device,
        mesh=split,
        in_specs=placed,
        out_specs=(P(None, GRP_LRN), P(LRN, None, None), P(LRN, None), P(LRN)),
        check_vma=False,
    )
```

```python
import math

import jax
import jax.numpy as jnp
from jax import lax
from jax.experimental import pallas as pl
from jax.experimental.pallas import tpu as pltpu
from jax.sharding import Mesh
from jax.sharding import PartitionSpec as P

MODES = 4
BINS = 64
G = 112
NB = 14
LEV = 32
COL_DEV = 128
LRN = ("x", "zl", "y")
GRP_LRN = ("zh", "cc", "x", "zl", "y")
MESH = pl.DeviceIdType.MESH
BF = jnp.bfloat16
F32 = jnp.float32
CLOUD_SSA = 0.99
CLOUD_ASYM = 0.85


def nt(a, b):
    return lax.dot_general(a, b, (((1,), (1,)), ((), ())), preferred_element_type=F32)


def nn(a, b):
    return jnp.dot(a, b, preferred_element_type=F32)


def iota(shape, dim):
    return lax.broadcasted_iota(jnp.int32, shape, dim)


def row_to_col(row):
    n = row.shape[1]
    rows = lax.broadcasted_iota(jnp.int32, (n, n), 0)
    cols = lax.broadcasted_iota(jnp.int32, (n, n), 1)
    return jnp.sum(jnp.where(rows == cols, jnp.broadcast_to(row, (n, n)), 0.0), axis=1, keepdims=True)


def evolve_setup(ext, ssa, asy, gas, sol, band, tab, gcol, m0):
    e = ext[...]
    s = e * ssa[...]
    tab[0:G, :] = e.astype(jnp.bfloat16)
    tab[G : 2 * G, :] = s.astype(jnp.bfloat16)
    tab[2 * G : 3 * G, :] = (s * asy[...]).astype(jnp.bfloat16)
    gcol[...] = jnp.broadcast_to(row_to_col(gas[...]), (G, COL_DEV))
    bcol = row_to_col(band[...].astype(jnp.float32))
    m0[...] = jnp.broadcast_to(jnp.where(bcol < NB // 2, 1.0, 0.0), (G, COL_DEV))
    return bcol


CH = 8
LU = 4


def evolve_layers(mass, bins, tau, mask, absb, tab, gcol, opt, refl, trans):
    labels = lax.broadcasted_iota(jnp.int32, (BINS, COL_DEV), 0)
    cloudy_on = mask[...].astype(jnp.float32)

    def body(step, carry):
        pieces = []
        for u in range(LU):
            l = step * LU + u
            modes = []
            for m in range(MODES):
                load = mass[m, pl.ds(l, 1), :]
                hot = bins[m, pl.ds(l, 1), :] == labels
                modes.append(jnp.where(hot, jnp.broadcast_to(load, (BINS, COL_DEV)), 0.0))
            pieces.append(jnp.concatenate(modes, axis=0).astype(jnp.bfloat16))
        weights = jnp.concatenate(pieces, axis=1)
        opt[...] = jnp.dot(tab[...], weights, preferred_element_type=jnp.float32)
        for u in range(LU):
            l = step * LU + u
            cl = tau[pl.ds(l, 1), :] * cloudy_on
            ab = absb[pl.ds(l, 1), :]
            c1 = CLOUD_SSA * cl
            c2 = CLOUD_SSA * CLOUD_ASYM * cl
            lanes = slice(u * COL_DEV, (u + 1) * COL_DEV)
            for g in range(0, G, CH):
                d = opt[g : g + CH, lanes] + cl + gcol[g : g + CH, :] * ab
                s = opt[G + g : G + g + CH, lanes] + c1
                f = opt[2 * G + g : 2 * G + g + CH, lanes] + c2
                ds, df = d - s, d - f
                k = 2.0 * jnp.sqrt(ds * df)
                g1 = ds + df
                e = jnp.exp(-k)
                sq = e * e
                r = 1.0 / ((k + g1) + (k - g1) * sq)
                refl[l, g : g + CH, :] = (s - f) * (1.0 - sq) * r
                trans[l, g : g + CH, :] = 2.0 * k * e * r
        return carry

    lax.fori_loop(0, LEV // LU, body, 0)


def evolve_up(alb, bcol, refl, trans, below):
    surface = jnp.zeros((G, COL_DEV), jnp.float32)
    for b in range(NB):
        surface = jnp.where(bcol == float(b), jnp.broadcast_to(alb[b : b + 1, :], (G, COL_DEV)), surface)
    below[LEV] = surface

    def body(step, carry):
        l = LEV - 1 - step
        layer = [(refl[l, g : g + CH, :], trans[l, g : g + CH, :]) for g in range(0, G, CH)]
        nxt, ratio = [], []
        for b, (r, t) in zip(carry, layer):
            q = t / (1.0 - r * b)
            ratio.append(q)
            nxt.append(r + t * b * q)
        for i, g in enumerate(range(0, G, CH)):
            below[l, g : g + CH, :] = nxt[i]
            trans[l, g : g + CH, :] = ratio[i]
        return tuple(nxt)

    lax.fori_loop(0, LEV, body, tuple(surface[g : g + CH, :] for g in range(0, G, CH)))


def evolve_down(sol, cosz, m0, below, trans, down, flux):
    cosv = cosz[...]
    scol = row_to_col(sol[...])
    down[...] = jnp.broadcast_to(scol, (G, COL_DEV)) * cosv
    scale = 2.0 / G

    def body(l, carry):
        acc = [jnp.zeros((CH, COL_DEV), jnp.float32) for _ in range(4)]
        for g in range(0, G, CH):
            rows = slice(g, g + CH)
            now = down[rows, :]
            low = m0[rows, :]
            up = below[l, rows, :] * now
            nxt = trans[l, rows, :] * now
            down[rows, :] = nxt
            nl, ul = nxt * low, up * low
            acc[0] = acc[0] + nl
            acc[1] = acc[1] + ul
            acc[2] = acc[2] + (nxt - nl)
            acc[3] = acc[3] + (up - ul)
        for i in range(4):
            flux[pl.ds(i * LEV + l, 1), :] = jnp.sum(acc[i], axis=0, keepdims=True) * scale
        return carry

    lax.fori_loop(0, LEV, body, 0)


EMPTY = 2.0
ROOT = math.sqrt(2.0 / math.pi)
CUBE = 0.044715


def remote(src, dst, send, recv, **at):
    return pltpu.make_async_remote_copy(
        src_ref=src, dst_ref=dst, send_sem=send, recv_sem=recv, device_id=at, device_id_type=MESH
    )


STEPS = sorted(
    ((dx, dy) for dx in range(4) for dy in range(8) if dx or dy),
    key=lambda s: (-min(s[0], 4 - s[0]) - min(s[1], 8 - s[1]), min(s[1], 8 - s[1]), s[0], s[1]),
)


def wait_bytes(ref, sem):
    pltpu.make_async_copy(ref, ref, sem).wait()


def send_features(mass, bins, lr, fs, slot_col):
    row = lr[...]
    col = row_to_col(row.astype(F32))
    same = jnp.broadcast_to(col, (COL_DEV, COL_DEV)) == jnp.broadcast_to(row.astype(F32), (COL_DEV, COL_DEV))
    before = iota((COL_DEV, COL_DEV), 0) < iota((COL_DEV, COL_DEV), 1)
    rank = jnp.sum(jnp.where(same & before, 1.0, 0.0), axis=0, keepdims=True).astype(jnp.int32)
    peer = (row >> 5) * 8 + (row & 7)
    key = peer * 16 + ((row >> 3) & 3) * 4 + rank
    slot_col[...] = peer * 8 + ((row >> 3) & 3) * 2 + rank
    first = ((jnp.log(mass[...]) + 4.6) / 1.4).reshape(MODES * LEV, COL_DEV).astype(BF)
    half = BINS / 2
    second = ((bins[...].astype(F32) - half) / half).reshape(MODES * LEV, COL_DEV).astype(BF)
    rows = iota((512, COL_DEV), 0)
    hot0 = jnp.where(rows == key, 1.0, 0.0).astype(BF)
    hot1 = jnp.where(rows == key + 2, 1.0, 0.0).astype(BF)
    data = nt(hot0, first) + nt(hot1, second)
    filled = nn(hot0 + hot1, jnp.ones((COL_DEV, COL_DEV), BF))
    empty = (filled < 0.5) & (iota((512, COL_DEV), 1) == 0)
    fs[...] = jnp.where(empty, EMPTY, data).reshape(32, 16, COL_DEV).astype(BF)


def kernel(
    mass_in, bins_in, tau_in, mask_in, absb_in, alb_in, cosz_in, ext_in, ssa_in, asy_in, gas_in, sol_in, band_in,
    lr_in, w_in, b_in, hw,
    flux, head, tg, bg,
    mass, bins, tau, mask, absb, alb, cosz, ext, ssa, asy, gas, sol, band, lr, w, b, in_sems,
    tab, gcol, m0, opt, refl, trans, below, down,
    slot_col, fs, fr, fz, fx, fo, ts, tr, tz, tx, to, wa, wb, wl, bs, br, bz, hv, hwt, biasc,
    xs, pre, slope, ht, pp, po, gt, ta, tps, bps, tpr, bpr, fsum, fbsum, gr, gb, hg,
    s_w, r_w, s_b, r_b, s_f, r_f, s_wz, r_wz, s_bz, r_bz, s_wl, r_wl, s_wy, r_wy, s_wx, r_wx, s_fz, r_fz, s_fd, r_fd,
    s_t, r_t, s_tz, r_tz, s_td, r_td, s_h, r_h, l_h, l_hw,
    s_k, r_k, s_kb, r_kb, s_e, r_e, s_eb, r_eb, s_p, r_p,
):
    zh, cc, x, zl, y = (lax.axis_index(a) for a in GRP_LRN)
    other = 1 - cc
    me = x * 8 + y
    z = zh * 4 + zl
    part = 2 * cc + zh
    own_piece = (part == x) & (x == zl)

    def plane(step):
        px, py = lax.rem(x + step[0], 4), lax.rem(y + step[1], 8)
        return px * 8 + py, px, py

    def ring(i):
        q = lax.rem(z + i, 8)
        return lax.div(q, 4), lax.rem(q, 4)

    pairs = [
        (lr_in, lr), (mass_in, mass), (bins_in, bins), (w_in, w), (b_in, b), (ext_in, ext), (ssa_in, ssa),
        (asy_in, asy), (gas_in, gas), (band_in, band), (tau_in, tau), (mask_in, mask), (absb_in, absb),
        (alb_in, alb), (cosz_in, cosz), (sol_in, sol),
    ]
    loads = [pltpu.make_async_copy(src, dst, in_sems.at[i]) for i, (src, dst) in enumerate(pairs)]
    barrier = pltpu.get_barrier_semaphore()

    for step in STEPS:
        _, px, py = plane(step)
        pl.semaphore_signal(barrier, inc=1, device_id={"x": px, "y": py}, device_id_type=MESH)
    for i in range(1, 8):
        qh, ql = ring(i)
        pl.semaphore_signal(barrier, inc=1, device_id={"zh": qh, "zl": ql}, device_id_type=MESH)
    pl.semaphore_signal(barrier, inc=1, device_id={"cc": other}, device_id_type=MESH)
    for a in range(4):

        @pl.when(jnp.logical_not(own_piece & (zl == a)))
        def _():
            at = {"zh": lax.rem(x, 2), "cc": lax.div(x, 2), "x": zl, "zl": a}
            pl.semaphore_signal(barrier, inc=1, device_id=at, device_id_type=MESH)

    for load in loads:
        load.start()
    hw_copy = pltpu.make_async_copy(hw.at[pl.ds(2 * cc, 2)], hv, l_hw)
    hw_copy.start()

    for load in loads[:5]:
        load.wait()
    send_features(mass, bins, lr, fs, slot_col)
    spread = (iota((16, COL_DEV), 1) == y * 16 + iota((16, COL_DEV), 0)).astype(BF)
    bs[...] = nn(b[...], spread)
    sender = lax.div(x, 2) == cc
    xb = lax.rem(x, 2)

    @pl.when(own_piece)
    def _():
        pl.semaphore_wait(barrier, 42)

    @pl.when(jnp.logical_not(own_piece))
    def _():
        pl.semaphore_wait(barrier, 43)

    z_steps = (1, 7, 2 + 4 * cc)

    @pl.when(sender)
    def _():
        for i in z_steps:
            qh, ql = ring(i)
            remote(w.at[:, COL_DEV:], wl.at[zl], s_wl, r_wl, zh=qh, zl=ql).start()
        wl[zl] = w[:, COL_DEV:]

    for step in STEPS:
        p, px, py = plane(step)
        remote(fs.at[p], fr.at[me], s_f, r_f, x=px, y=py).start()
    fr[me] = fs[me]

    @pl.when(sender)
    def _():
        for step in STEPS:
            _, px, py = plane(step)
            remote(w.at[:, 0:COL_DEV], wa.at[xb, zl, y], s_w, r_w, x=px, y=py).start()
            remote(bs, br.at[xb, y], s_b, r_b, x=px, y=py).start()
        wa[xb, zl, y] = w[:, 0:COL_DEV]
        br[xb, y] = bs[...]

    for load in loads[5:]:
        load.wait()
    bcol = evolve_setup(ext, ssa, asy, gas, sol, band, tab, gcol, m0)
    evolve_layers(mass, bins, tau, mask, absb, tab, gcol, opt, refl, trans)

    @pl.when(sender)
    def _():
        wait_bytes(fr.at[0:3], r_wl)
        for i in range(1, 8):
            remote(wl, wb.at[xb, :, y], s_wy, r_wy, y=lax.rem(y + i, 8)).start()
        wb[xb, :, y] = wl[...]

    wait_bytes(fr.at[0:31], r_f)
    got = fr[...].reshape(512, COL_DEV)
    o = iota((COL_DEV, 512), 0)
    source = ((o >> 1) & 31) * 16 + (o >> 6) * 2 + (o & 1)
    shift = iota((COL_DEV, 512), 1) - source
    for a in range(4):
        pick = jnp.where(shift == 4 * a, 1.0, 0.0).astype(BF)
        fz[a] = nn(pick, got).astype(BF)
    for i in (4, 3, 5, 2, 6, 1, 7):
        qh, ql = ring(i)
        remote(fz.at[ql], fx.at[z], s_fz, r_fz, zh=qh, zl=ql).start()
    fx[z] = fz[zl]

    evolve_up(alb, bcol, refl, trans, below)
    evolve_down(sol, cosz, m0, below, trans, down, flux)

    place = jnp.where(iota((256, COL_DEV), 0) == slot_col[...], 1.0, 0.0).astype(BF)
    ts[...] = nt(place, flux[...].astype(BF)).reshape(32, 8, COL_DEV).astype(BF)

    for step in STEPS:
        p, px, py = plane(step)
        remote(ts.at[p], tr.at[me], s_t, r_t, x=px, y=py).start()
    tr[me] = ts[me]

    @pl.when(sender)
    def _():
        wait_bytes(fr.at[0:15], r_w)
        wait_bytes(bpr.at[0:15], r_b)

    @pl.when(jnp.logical_not(sender))
    def _():
        wait_bytes(fr.at[0:16], r_w)
        wait_bytes(bpr.at[0:16], r_b)

    for a in range(2):
        bz[a, zl] = jnp.sum(br[a], axis=0)
    for i in z_steps:
        qh, ql = ring(i)
        remote(wa.at[:, zl], wa.at[:, zl], s_wz, r_wz, zh=qh, zl=ql).start()
        remote(bz.at[:, zl], bz.at[:, zl], s_bz, r_bz, zh=qh, zl=ql).start()

    @pl.when(sender)
    def _():
        wait_bytes(fr.at[0:28], r_wy)
        for i in (1, 3, 2):
            remote(wb.at[xb], wb.at[xb], s_wx, r_wx, x=lax.rem(x + i, 4)).start()

    hw_copy.wait()
    eye = jnp.where(iota((COL_DEV, COL_DEV), 0) == iota((COL_DEV, COL_DEV), 1), 1.0, 0.0).astype(BF)
    for a in range(2):
        hwt[a] = (0.5 * nt(eye, hv[a])).astype(BF)
    wait_bytes(tr.at[0:31], r_t)
    gott = tr[...].astype(F32).reshape(256, COL_DEV).astype(BF)
    ot = iota((64, 256), 0)
    shift_t = iota((64, 256), 1) - ((ot >> 1) * 8 + (ot & 1))
    for a in range(4):
        tz[a] = nn(jnp.where(shift_t == 2 * a, 1.0, 0.0).astype(BF), gott).astype(BF)
    for i in (4, 3, 5, 2, 6, 1, 7):
        qh, ql = ring(i)
        remote(tz.at[ql], tx.at[z], s_tz, r_tz, zh=qh, zl=ql).start()
    tx[z] = tz[zl]

    wait_bytes(fx.at[0:7], r_fz)
    fd = remote(fx, fo, s_fd, r_fd, cc=other)
    fd.start()
    wait_bytes(bz.at[:, 0:3], r_bz)
    for a in range(2):
        for q in range(4):
            biasc[a, q * COL_DEV : (q + 1) * COL_DEV, :] = jnp.broadcast_to(row_to_col(bz[a, q]), (COL_DEV, COL_DEV))
    wait_bytes(wa.at[:, 0:3], r_wz)

    @pl.when(sender)
    def _():
        wait_bytes(wb.at[0], r_wx)

    @pl.when(jnp.logical_not(sender))
    def _():
        wait_bytes(wb, r_wx)

    def gather_x(side, ref):
        for q in range(8):
            for h in range(2):
                xs[side * 2 + q // 4, (q % 4) * 64 : (q % 4 + 1) * 64, h * COL_DEV : (h + 1) * COL_DEV] = ref[
                    q, h * 64 : (h + 1) * 64, :
                ]

    gather_x(0, fx)

    def forward(sb, half, with_slope):
        rows = jnp.concatenate([wa[half].reshape(512, COL_DEV), wb[half].reshape(512, COL_DEV)], axis=1)
        pre[...] = nt(rows, xs[sb])
        for r in range(0, 512, 32):
            v = pre[r : r + 32, :]
            bc = biasc[half, r : r + 32, :]
            v = v + jnp.concatenate([bc, bc], axis=1)
            sq = v * v
            t = jnp.tanh(v * (ROOT + (ROOT * CUBE) * sq))
            up = 1.0 + t
            ht[sb, half, r : r + 32, :] = (v * up).astype(BF)
            if with_slope:
                slope[sb, r : r + 32, :] = up + v * ((1.0 - t * t) * (ROOT + (3.0 * CUBE * ROOT) * sq))
        return nn(hwt[half], ht[sb, half])

    def swap(sb):
        return remote(pp.at[sb], po.at[sb], s_p.at[sb], r_p.at[sb], cc=other)

    def forward_block(sb, c):
        pp[sb] = forward(sb, zh, True) + forward(sb, 1 - zh, False)
        swap(sb).start()
        return c

    lax.fori_loop(0, 2, forward_block, 0)
    fd.wait()
    gather_x(1, fo)
    lax.fori_loop(2, 3, forward_block, 0)
    wait_bytes(tx.at[0:7], r_tz)
    td = remote(tx, to, s_td, r_td, cc=other)
    td.start()
    lax.fori_loop(3, 4, forward_block, 0)
    lane0 = jnp.where(iota((8, COL_DEV), 1) == 0, 1.0, 0.0).astype(BF)

    def pred_grad(sb):
        src = (tx, tx, to, to)[sb]
        goal = nt(eye, src[(sb % 2) * 4 : (sb % 2) * 4 + 4].reshape(256, COL_DEV))
        flag = nt(lane0, xs[sb, :, COL_DEV:])[0:1, :]
        factor = jnp.where(flag < 1.5, 1.0 / COL_DEV, 0.0)
        gt[sb] = (((pp[sb] + po[(sb + 2) % 4]) - goal) * factor).astype(BF)

    ones = jnp.ones((8, 256), BF)

    def backward(sb, units):
        hgrad = nn(hv[zh, units, :], gt[sb])
        pgrad = ((0.5 * hgrad) * slope[sb, units, :]).astype(BF)
        return nn(pgrad, xs[sb]), nt(ones, pgrad)

    td.wait()
    for sb in (2, 3):
        swap(sb - 2).wait_recv()
        pred_grad(sb)
    brows = []
    for part_of in range(2):
        units = slice(part_of * 256, part_of * 256 + 256)
        term, brow = backward(2, units)
        ta[units, :] = term
        term, more = backward(3, units)
        ta[units, :] = ta[units, :] + term
        brows.append(brow + more)
    for sb in (0, 1):
        swap(sb + 2).wait_recv()
        pred_grad(sb)
    for px in range(4):
        units = slice(px * COL_DEV, px * COL_DEV + COL_DEV)
        brow = brows[px // 2][:, (px % 2) * COL_DEV : (px % 2 + 1) * COL_DEV]
        for sb in (0, 1):
            term, more = backward(sb, units)
            ta[units, :] = ta[units, :] + term
            brow = brow + more
        tps[px * 8 : px * 8 + 8] = ta[units, :].reshape(8, 16, 256).astype(BF)
        bps[px] = brow[0:1, :]
        for dy in (4, 3, 5, 2, 6, 1, 7, 0):
            py = lax.rem(y + dy, 8)
            p = px * 8 + py

            def send(p=p, px=px, py=py):
                remote(tps.at[p], tpr.at[me], s_k, r_k, x=px, y=py).start()
                remote(bps.at[px], bpr.at[me], s_kb, r_kb, x=px, y=py).start()

            if dy:
                send()
            else:
                pl.when(x != px)(send)

    tpr[me] = tps[me]
    bpr[me] = bps[x]

    for half in range(2):
        total = nt(ht[0, half], gt[0])
        for sb in range(1, 4):
            total = total + nt(ht[sb, half], gt[sb])
        hg[half] = 0.5 * total
    hd = remote(hg, head.at[pl.ds(2 * cc, 2)], s_h, r_h, cc=other)
    hd.start()
    hl = pltpu.make_async_copy(hg, head.at[pl.ds(2 * cc, 2)], l_h)
    hl.start()

    wait_bytes(tpr.at[0:31], r_k)
    wait_bytes(bpr.at[0:31], r_kb)
    fsum[...] = jnp.sum(tpr[...].astype(F32), axis=0)
    fbsum[...] = jnp.sum(bpr[...], axis=0)
    for qh in range(2):
        for qc in range(2):
            mine = own_piece & (zh == qh) & (cc == qc)

            @pl.when(jnp.logical_not(mine))
            def _():
                at = dict(zh=qh, cc=qc, x=part, zl=x)
                remote(fsum, gr.at[zl], s_e, r_e, **at).start()
                remote(fbsum, gb.at[zl], s_eb, r_eb, **at).start()

            @pl.when(mine)
            def _():
                gr[zl] = fsum[...]
                gb[zl] = fbsum[...]

    @pl.when(own_piece)
    def _():
        wait_bytes(gr.at[0:3], r_e)
        wait_bytes(gb.at[0:3], r_eb)

    @pl.when(jnp.logical_not(own_piece))
    def _():
        wait_bytes(gr, r_e)
        wait_bytes(gb, r_eb)

    tg[...] = (gr[0] + gr[1]) + (gr[2] + gr[3])
    brows = (gb[0] + gb[1]) + (gb[2] + gb[3])
    kept = jnp.where(lax.div(iota((1, COL_DEV), 1), 16) == y, brows, 0.0)
    bias = kept[:, 0:16]
    for a in range(1, 8):
        bias = bias + kept[:, a * 16 : (a + 1) * 16]
    bg[...] = bias

    hl.wait()
    hd.wait_send()
    for sb in range(4):
        swap(sb).wait_send()
    wait_bytes(head.at[pl.ds(2 * other, 2)], r_h)

    @pl.when(sender)
    def _():
        wait_bytes(fr.at[0:31], s_w)
        wait_bytes(bpr.at[0:31], s_b)
        wait_bytes(fr.at[0:3], s_wl)
        wait_bytes(fr.at[0:28], s_wy)
        wait_bytes(xs.at[0:3], s_wx)

    wait_bytes(fs.at[0:31], s_f)
    wait_bytes(wa.at[:, 0:3], s_wz)
    wait_bytes(bz.at[:, 0:3], s_bz)
    wait_bytes(fx.at[0:7], s_fz)
    wait_bytes(ts.at[0:31], s_t)
    wait_bytes(tx.at[0:7], s_tz)
    wait_bytes(tps.at[0:31], s_k)
    wait_bytes(bpr.at[0:31], s_kb)

    @pl.when(own_piece)
    def _():
        wait_bytes(gr.at[0:3], s_e)
        wait_bytes(gb.at[0:3], s_eb)

    @pl.when(jnp.logical_not(own_piece))
    def _():
        wait_bytes(gr, s_e)
        wait_bytes(gb, s_eb)


def copy_out(flux_in, head_in, tg_in, bg_in, flux, head, tg, bg, vflux, vhead, vtg, vbg, sems):
    trips = [(head_in.at[i], vhead.at[i], head.at[i]) for i in range(4)]
    trips += [(flux_in, vflux, flux), (tg_in, vtg, tg), (bg_in, vbg, bg)]
    ins = [pltpu.make_async_copy(a, b, sems.at[0, i]) for i, (a, b, _) in enumerate(trips)]
    outs = [pltpu.make_async_copy(b, c, sems.at[1, i]) for i, (_, b, c) in enumerate(trips)]
    for copy in ins:
        copy.start()
    for copy, out in zip(ins, outs):
        copy.wait()
        out.start()
    for out in outs:
        out.wait()


def per_device(mass, bins, tau, mask, absb, alb, cosz, ext, ssa, asy, gas, sol, band, lr, w, b, hw):
    vm = pl.BlockSpec(memory_space=pltpu.VMEM)
    hbm = pl.BlockSpec(memory_space=pl.ANY)
    v = pltpu.VMEM
    c = COL_DEV
    flux, head, tg, bg = pl.pallas_call(
        kernel,
        out_shape=(
            jax.ShapeDtypeStruct((4 * LEV, c), F32),
            jax.ShapeDtypeStruct((4, 512, c), F32),
            jax.ShapeDtypeStruct((16, 256), F32),
            jax.ShapeDtypeStruct((1, 16), F32),
        ),
        in_specs=[hbm] * 17,
        out_specs=(vm, hbm, vm, vm),
        scratch_shapes=[
            v((MODES, LEV, c), F32), v((MODES, LEV, c), jnp.int32), v((LEV, c), F32), v((1, c), jnp.int32),
            v((LEV, c), F32), v((NB, c), F32), v((1, c), F32), v((G, 256), F32), v((G, 256), F32), v((G, 256), F32),
            v((1, G), F32), v((1, G), F32), v((1, G), jnp.int32), v((1, c), jnp.int32), v((16, 256), BF), v((1, 16), BF),
            pltpu.SemaphoreType.DMA((16,)),
            v((3 * G, MODES * BINS), BF), v((G, c), F32), v((G, c), F32), v((3 * G, LU * c), F32),
            v((LEV, G, c), F32), v((LEV, G, c), F32), v((LEV + 1, G, c), F32), v((G, c), F32),
            v((1, c), jnp.int32),
            v((32, 16, c), BF), v((32, 16, c), BF), v((4, 128, c), BF), v((8, 128, c), BF), v((8, 128, c), BF),
            v((32, 8, c), BF), v((32, 8, c), BF), v((4, 64, c), BF), v((8, 64, c), BF), v((8, 64, c), BF),
            v((2, 4, 8, 16, c), BF), v((2, 4, 8, 16, c), BF), v((4, 16, c), BF), v((1, c), F32), v((2, 8, 1, c), F32), v((2, 4, 1, c), F32),
            v((2, 512, c), BF), v((2, c, 512), BF), v((2, 512, c), F32),
            v((4, 256, 256), BF), v((512, 256), F32), v((4, 512, 256), F32), v((4, 2, 512, 256), BF),
            v((4, c, 256), F32), v((4, c, 256), F32), v((4, c, 256), BF), v((512, 256), F32),
            v((32, 16, 256), BF), v((4, 1, c), F32), v((32, 16, 256), BF), v((32, 1, c), F32),
            v((16, 256), F32), v((1, c), F32), v((4, 16, 256), F32), v((4, 1, c), F32), v((2, 512, c), F32),
        ] + [pltpu.SemaphoreType.DMA] * 38 + [pltpu.SemaphoreType.DMA((4,))] * 2,
        compiler_params=pltpu.CompilerParams(collective_id=0, has_side_effects=True),
    )(
        mass, bins, tau, mask[None], absb, alb, cosz[None], ext, ssa, asy, gas[None], sol[None], band[None],
        lr.reshape(1, c), w, b[None], hw.reshape(4, 512, c),
    )
    flux, head, tg, bg = pl.pallas_call(
        copy_out,
        out_shape=tuple(jax.ShapeDtypeStruct(a.shape, F32) for a in (flux, head, tg, bg)),
        in_specs=[hbm] * 4,
        out_specs=(hbm,) * 4,
        scratch_shapes=[v(a.shape, F32) for a in (flux, head, tg, bg)] + [pltpu.SemaphoreType.DMA((2, 7))],
    )(flux, head, tg, bg)
    return flux, head.reshape(1, 2048, c), tg, bg[0]


def solution(mesh):
    split = Mesh(mesh.devices.reshape(2, 2, 4, 4, 8), GRP_LRN)
    placed = (
        P(None, None, GRP_LRN),
        P(None, None, GRP_LRN),
        P(None, GRP_LRN),
        P(GRP_LRN),
        P(None, GRP_LRN),
        P(None, GRP_LRN),
        P(GRP_LRN),
        P(),
        P(),
        P(),
        P(),
        P(),
        P(),
        P(GRP_LRN, None),
        P(LRN, None),
        P(LRN),
        P(LRN, None, None),
    )
    return jax.shard_map(
        per_device,
        mesh=split,
        in_specs=placed,
        out_specs=(P(None, GRP_LRN), P(LRN, None, None), P(LRN, None), P(LRN)),
        check_vma=False,
    )
```
